32 devices in a mesh: blk: 16 (over z, y, core), head: 2 (over x).
Axes of the slice: x: 2, y: 2, z: 4, core: 2. Of those that a mesh axis runs over, the one named last changes fastest.
Arguments:
- queries: bfloat16 [4096, 1024], P('blk', 'head'), may hold values from -216 to 216
- keys: bfloat16 [4096, 1024], P('blk', 'head'), may hold values from -6 to 6
- values: bfloat16 [4096, 1024], P('blk', 'head'), may hold values from -6 to 6
- group_table: int32 [16, 2], P('blk'), may hold values from 0 to 31, as said below
- doc_ids: int32 [4096], replicated, may hold values from 0 to 15, never falling along the last dimension, each value on 1 to 2048 neighbouring positions
Outputs:
- attended: bfloat16 [4096, 1024], P('blk', 'head')
The draws below stay inside these ranges and needn't reach their ends.
Inputs may be any that keep to these rules, and one draw needn't show every extreme that they name: group_table[d, 1] = 31 - group_table[d, 0]; the first column holds each of 0 to 15 once. `doc_ids`: document numbers never fall along positions; a document holds at most 2048 positions.
All inputs are finite; a program needn't handle non-finite values.
Results may differ from the reference program's by a relative error of at most 0.0049.
Values may be sent and summed in bfloat16 or wider, within the bound.
A program may use at most 192 MiB of HBM per device.

```python
import math
import jax
import jax.numpy as jnp
import numpy as np
from jax import lax

HEAD_DIM = 128
HEADS = 8
TOK_DEV = 256
DOCS = 16
GROUP = 128
SEQ = 4096
MAXDOC = 2048
N_BLK = 16


def draw_queries(key, part):
    drawn = jnp.clip(jax.random.normal(jax.random.fold_in(key, 11), (SEQ, HEADS, HEAD_DIM), jnp.float32), -6.0, 6.0)
    return drawn.reshape(SEQ, HEADS * HEAD_DIM).astype(jnp.bfloat16)


def draw_keys(key, part):
    drawn = jnp.clip(jax.random.normal(jax.random.fold_in(key, 13), (SEQ, HEADS, HEAD_DIM), jnp.float32), -6.0, 6.0)
    return drawn.reshape(SEQ, HEADS * HEAD_DIM).astype(jnp.bfloat16)


def draw_group_table(key, part):
    order = jax.random.permutation(jax.random.fold_in(key, 17), N_BLK).astype(jnp.int32)
    return jnp.stack([order, 2 * N_BLK - 1 - order], axis=1).astype(jnp.int32)


def steps_of(key, extent, pieces, low, high):
    def one(dim, shards_of):
        heights = jax.random.uniform(jax.random.fold_in(jax.random.fold_in(key, 6), dim), (shards_of,), jnp.float32, low / len(pieces), high / len(pieces))
        return jnp.repeat(jnp.exp(heights), extent[dim] // shards_of).reshape((-1,) + (1,) * (len(extent) - dim - 1))

    loudness = one(*pieces[0])
    for cut in pieces[1:]:
        loudness = loudness * one(*cut)
    return loudness


def length_profile(amount, total, most, slope):
    loads = [(1 << 20) // math.isqrt(grade ** slope) + 1 for grade in range(2, amount + 1)]
    surplus, holding = total - most - (amount - 1), [1] * (amount - 1)
    while surplus > 0:
        candidates = [i for i in range(amount - 1) if holding[i] < most]
        whole, remaining = sum([loads[i] for i in candidates]), surplus
        for i in candidates:
            extra = min(most - holding[i], max(1, remaining * loads[i] // whole), surplus)
            holding[i] = holding[i] + extra
            surplus = surplus - extra
    return np.array([most] + holding)


def uneven(stream_key, count, total, most, slope):
    if count == 2:
        one = jax.random.randint(stream_key, (), max(1, total - most), min(most, total - 1) + 1)
        return jnp.stack([one, total - one])
    tallies = jnp.asarray(length_profile(count, total, most, slope), jnp.int32)
    twos = (count - 1) // 2
    donor, taker = tallies[1:1 + 2 * twos:2], tallies[2:2 + 2 * twos:2]
    margin = jnp.minimum(donor - 1, most - taker)
    passed = jax.random.randint(jax.random.fold_in(stream_key, 1), (twos,), 0, 1 << 20) % (margin + 1)
    tallies = tallies.at[1:1 + 2 * twos:2].set(donor - passed).at[2:2 + 2 * twos:2].set(taker + passed)
    return tallies[jax.random.permutation(jax.random.fold_in(stream_key, 2), count)]


def noise(rng, extent, deviation, reach, pieces=(), kind=jnp.bfloat16):
    values = jax.random.normal(rng, extent, jnp.float32) * deviation
    if len(pieces) > 0:
        values = steps_of(rng, extent, pieces, -0.22, 0.18) * values
    return jnp.clip(values, min=-reach, max=reach).astype(kind)


def setup_inputs(seed: int = 0) -> dict:
    streams_of = jax.random.split(jax.random.key(seed), 6)
    return {
        "queries": draw_queries(jax.random.fold_in(streams_of[5], 71), 0),
        "keys": draw_keys(jax.random.fold_in(streams_of[5], 71), 0),
        "values": noise(streams_of[2], (SEQ, HEADS * HEAD_DIM), 1.0, 6.0, ((0, 16), (1, 2))),
        "group_table": draw_group_table(jax.random.fold_in(streams_of[5], 71), 0),
        "doc_ids": jnp.searchsorted(jnp.cumsum(uneven(streams_of[4], DOCS, SEQ, MAXDOC, 2)), jnp.arange(SEQ), side="right").astype(jnp.int32),
    }


def reference(queries, keys, values, group_table, doc_ids):
    row_ids = jnp.arange(SEQ, dtype=jnp.int32)
    device = row_ids // TOK_DEV
    slot_ids = row_ids % TOK_DEV // GROUP
    position = (group_table[device, slot_ids] * GROUP + row_ids % GROUP).astype(jnp.int32)
    document = doc_ids[position]
    score_scale = 1.0 / math.sqrt(HEAD_DIM)
    query_block = math.gcd(SEQ, 1024)
    block_count = SEQ // query_block

    def one_head(head_index):
        start = (head_index * HEAD_DIM).astype(jnp.int32)
        head_queries = lax.dynamic_slice_in_dim(queries, start, HEAD_DIM, 1)
        head_keys = lax.dynamic_slice_in_dim(keys, start, HEAD_DIM, 1)
        head_values = lax.dynamic_slice_in_dim(values, start, HEAD_DIM, 1)

        def attend_block(args):
            query_rows, block_pos, block_doc = args
            scores = jnp.dot(query_rows, head_keys.T, preferred_element_type=jnp.float32) * score_scale
            visible = (block_doc[:, None] == document[None, :]) & (position[None, :] <= block_pos[:, None])
            rowmax = lax.optimization_barrier(jnp.max(jnp.where(visible, scores, -jnp.inf), axis=1))
            weights = jnp.where(visible, jnp.exp(scores - rowmax[:, None]), 0.0)
            denominator = lax.optimization_barrier(jnp.sum(weights, axis=1))
            output = jnp.dot(weights.astype(jnp.bfloat16), head_values, preferred_element_type=jnp.float32)
            return output / denominator[:, None]
        blocks = (head_queries.reshape(block_count, query_block, HEAD_DIM), position.reshape(block_count, query_block), document.reshape(block_count, query_block))
        return lax.map(attend_block, blocks).reshape(SEQ, HEAD_DIM)
    outputs = lax.map(one_head, jnp.arange(HEADS, dtype=jnp.int32))
    return jnp.transpose(outputs, (1, 0, 2)).reshape(SEQ, HEADS * HEAD_DIM).astype(jnp.bfloat16)
```

```python
import functools
import math

import jax
import jax.numpy as jnp
from jax import lax
from jax.experimental import pallas as pl
from jax.experimental.pallas import tpu as pltpu
from jax.sharding import PartitionSpec as P

HEAD_DIM = 128
CORES = 2
MASKED = -1e30


def attend_kernel(
    cells, table_ref, q_hbm, k_hbm, v_hbm, doc_ref, out_ref,
    stage_q, stage_kv, qin, kv, meta, osend, ssend, obuf, sbuf,
    load_q, load_kv, own_sem, q_send, q_recv, kv_send, kv_recv, fwd_send, m_send, m_recv, mf_send,
    o_send, o_recv, s_send, s_recv,
):
    rows, cols = q_hbm.shape
    heads = cols // HEAD_DIM
    group = rows // 2
    factor = math.log2(math.e) / math.sqrt(HEAD_DIM)
    me = lax.axis_index("blk")
    core = lax.rem(me, CORES)
    chip = lax.rem(me // CORES, heads)
    cell = me // (CORES * heads)

    def index(cc, ch, co):
        return (cc * heads + ch) * CORES + co

    partner = index(cell, chip, 1 - core)

    def head_columns(h):
        start = h * HEAD_DIM
        if not isinstance(h, int):
            start = pl.multiple_of(start, HEAD_DIM)
        return pl.ds(start, HEAD_DIM)

    def own_slot(ch, co):
        return ch * CORES + co

    q_loads = [pltpu.make_async_copy(q_hbm.at[:, head_columns(h)], stage_q.at[h], load_q.at[h]) for h in range(heads)]
    kv_loads = []
    for h in range(heads):
        kv_loads.append((
            pltpu.make_async_copy(k_hbm.at[:, head_columns(h)], stage_kv.at[h, :, pl.ds(0, HEAD_DIM)], load_kv.at[h, 0]),
            pltpu.make_async_copy(v_hbm.at[:, head_columns(h)], stage_kv.at[h, :, pl.ds(HEAD_DIM, HEAD_DIM)], load_kv.at[h, 1]),
        ))
    own_kv = (
        pltpu.make_async_copy(k_hbm.at[:, head_columns(chip)], kv.at[own_slot(chip, core), :, pl.ds(0, HEAD_DIM)], own_sem.at[0]),
        pltpu.make_async_copy(v_hbm.at[:, head_columns(chip)], kv.at[own_slot(chip, core), :, pl.ds(HEAD_DIM, HEAD_DIM)], own_sem.at[1]),
    )
    own_q = pltpu.make_async_copy(q_hbm.at[:, head_columns(chip)], qin.at[cell, chip], own_sem.at[2])
    for one in q_loads:
        one.start()
    for pair in kv_loads:
        for one in pair:
            one.start()
    for one in own_kv:
        one.start()
    own_q.start()

    barrier = pltpu.get_barrier_semaphore()
    peers = []
    for k in range(cells):
        for i in range(heads):
            if k or i:
                peers.append((lax.rem(cell + k, cells), lax.rem(chip + i, heads), k * heads + i))
    for cc, ch, _ in peers:
        pl.semaphore_signal(barrier, inc=1, device_id={"blk": index(cc, ch, core)})
    pl.semaphore_signal(barrier, inc=1, device_id={"blk": partner})

    within = lax.broadcasted_iota(jnp.int32, (1, group), 1)
    for g in range(2):
        own_group = table_ref[0, g]
        meta[me, pl.ds(g, 1), :] = doc_ref[pl.ds(own_group, 1), :]
        meta[me, pl.ds(2 + g, 1), :] = own_group * group + within

    pl.semaphore_wait(barrier, len(peers) + 1)

    def remote(src, dst, ssem, rsem, target):
        return pltpu.make_async_remote_copy(
            src_ref=src, dst_ref=dst, send_sem=ssem, recv_sem=rsem, device_id={"blk": target}
        )

    def q_copy(cc, ch, n):
        return remote(stage_q.at[ch], qin.at[cell, chip], q_send.at[n], q_recv.at[cell, chip], index(cc, ch, core))

    def kv_copy(ch, n):
        place = own_slot(chip, core)
        return remote(stage_kv.at[ch], kv.at[place], kv_send.at[n], kv_recv.at[place], index(cell, ch, core))

    def kv_forward(ch):
        place = own_slot(ch, core)
        return remote(kv.at[place], kv.at[place], fwd_send.at[ch], kv_recv.at[place], partner)

    def meta_copy(cc, ch, n):
        return remote(meta.at[me], meta.at[me], m_send.at[n], m_recv.at[me], index(cc, ch, core))

    def meta_forward(ch):
        source = index(cell, ch, core)
        return remote(meta.at[source], meta.at[source], mf_send.at[ch], m_recv.at[source], partner)

    def q_arrival(cc, ch):
        return remote(stage_q.at[0], qin.at[cc, ch], q_send.at[0], q_recv.at[cc, ch], partner)

    def kv_arrival(place):
        return remote(kv.at[place], kv.at[place], fwd_send.at[0], kv_recv.at[place], partner)

    def meta_arrival(source):
        return remote(meta.at[source], meta.at[source], mf_send.at[0], m_recv.at[source], partner)

    near = [one for one in peers if one[2] < heads]
    far = [one for one in peers if one[2] >= heads]
    for one in q_loads:
        one.wait()
    for cc, ch, n in near:
        q_copy(cc, ch, n).start()
    for pair in kv_loads:
        for one in pair:
            one.wait()
    for cc, ch, n in near:
        kv_copy(ch, n).start()
    for cc, ch, n in near:
        meta_copy(cc, ch, n).start()
    for cc, ch, n in far:
        q_copy(cc, ch, n).start()
    for cc, ch, n in far:
        meta_copy(cc, ch, n).start()
    for one in own_kv:
        one.wait()
    kv_forward(chip).start()
    meta_forward(chip).start()
    own_q.wait()
    for cc, ch, n in near:
        kv_arrival(own_slot(ch, core)).wait_recv()
        kv_forward(ch).start()
        meta_arrival(index(cell, ch, core)).wait_recv()
        meta_forward(ch).start()
    for i in range(heads):
        ch = lax.rem(chip + i, heads)
        kv_arrival(own_slot(ch, 1 - core)).wait_recv()
        meta_arrival(index(cell, ch, 1 - core)).wait_recv()

    sources = heads * CORES
    key_doc = [[meta[cell * sources + s, pl.ds(g, 1), :] for s in range(sources)] for g in range(2)]
    key_pos = [[meta[cell * sources + s, pl.ds(2 + g, 1), :] for s in range(sources)] for g in range(2)]
    down = lax.broadcasted_iota(jnp.int32, (group, group), 0)
    right = lax.broadcasted_iota(jnp.int32, (group, group), 1)
    diagonal = down == right

    def to_rows(line):
        return jnp.sum(jnp.where(diagonal, line, 0), axis=1, keepdims=True)

    def to_lanes(column):
        return jnp.sum(jnp.where(diagonal, column, 0), axis=0, keepdims=True)

    def attend(q, source, slot):
        doc = jnp.broadcast_to(to_rows(meta[source, pl.ds(slot, 1), :]), (group, group))
        pos = jnp.broadcast_to(to_rows(meta[source, pl.ds(2 + slot, 1), :]), (group, group))
        parts = []
        for g in range(slot + 1):
            keys = kv[:, pl.ds(g * group, group), pl.ds(0, HEAD_DIM)].reshape(sources * group, HEAD_DIM)
            scores = lax.dot_general(q, keys, (((1,), (1,)), ((), ())), preferred_element_type=jnp.float32)
            for s in range(sources):
                seen = (key_doc[g][s] == doc) & (key_pos[g][s] <= pos)
                parts.append(jnp.where(seen, scores[:, s * group:(s + 1) * group], MASKED))
        best = parts[0]
        for one in parts[1:]:
            best = jnp.maximum(best, one)
        best = jnp.broadcast_to(jnp.max(best, axis=1, keepdims=True), (group, group))
        total = None
        out = None
        for g in range(slot + 1):
            weights = [jnp.exp2((one - best) * factor) for one in parts[g * sources:(g + 1) * sources]]
            for one in weights:
                total = one if total is None else total + one
            weights = jnp.concatenate([one.astype(jnp.bfloat16) for one in weights], axis=1)
            vals = kv[:, pl.ds(g * group, group), pl.ds(HEAD_DIM, HEAD_DIM)].reshape(sources * group, HEAD_DIM)
            add = jnp.dot(weights, vals, preferred_element_type=jnp.float32)
            out = add if out is None else out + add
        total = jnp.broadcast_to(jnp.sum(total, axis=1, keepdims=True), (group, group))
        return out, to_lanes(best), to_lanes(total)

    def o_copy(cc, ch, n):
        return remote(osend.at[n], obuf.at[cell, chip], o_send.at[n], o_recv.at[cell, chip], index(cc, ch, core))

    def s_copy(cc, ch, n):
        return remote(ssend.at[n], sbuf.at[cell, chip], s_send.at[n], s_recv.at[cell, chip], index(cc, ch, core))

    def o_arrival(cc, h):
        return remote(osend.at[0], obuf.at[cc, h], o_send.at[0], o_recv.at[cc, h], partner)

    def s_arrival(cc, h):
        return remote(ssend.at[0], sbuf.at[cc, h], s_send.at[0], s_recv.at[cc, h], partner)

    def place_of(t):
        return lax.rem(cell + 1 + t // heads, cells), lax.rem(chip + lax.rem(t, heads), heads)

    def serve(t, carry):
        cc, ch = place_of(t)
        home = index(cc, ch, core)
        other = home != me

        def arrive():
            q_arrival(cc, ch).wait_recv()

        pl.when(other)(arrive)

        def arrive_meta():
            meta_arrival(home).wait_recv()

        pl.when(cc != cell)(arrive_meta)
        for slot in range(2):
            q = qin[cc, ch, pl.ds(slot * group, group), :]
            out, best, total = attend(q, home, slot)
            osend[t, pl.ds(slot * group, group), :] = out.astype(jnp.bfloat16)
            ssend[t, pl.ds(slot, 1), :] = best
            ssend[t, pl.ds(2 + slot, 1), :] = total

        def give():
            o_copy(cc, ch, t).start()
            s_copy(cc, ch, t).start()

        pl.when(other)(give)
        return carry

    lax.fori_loop(0, cells * heads, serve, 0)

    own_turn = (cells - 1) * heads
    obuf[cell, chip] = osend[own_turn]
    sbuf[cell, chip] = ssend[own_turn]

    for h in range(heads):
        column = pl.ds(h * HEAD_DIM, HEAD_DIM)
        for cc in range(cells):
            def arrive_partial():
                o_arrival(cc, h).wait_recv()
                s_arrival(cc, h).wait_recv()

            pl.when((cell != cc) | (chip != h))(arrive_partial)
        for slot in range(2):
            part = pl.ds(slot * group, group)
            tops = [sbuf[cc, h, pl.ds(slot, 1), :] for cc in range(cells)]
            sums = [sbuf[cc, h, pl.ds(2 + slot, 1), :] for cc in range(cells)]
            top = functools.reduce(jnp.maximum, tops)
            scale = [jnp.exp2((one - top) * factor) for one in tops]
            total = functools.reduce(jnp.add, [a * b for a, b in zip(scale, sums)])
            mixed = None
            for cc in range(cells):
                weight = to_rows(scale[cc] / total)
                term = obuf[cc, h, part, :].astype(jnp.float32) * weight
                mixed = term if mixed is None else mixed + term
            out_ref[part, column] = mixed.astype(out_ref.dtype)

    for cc, ch, n in peers:
        q_copy(cc, ch, n).wait_send()
        meta_copy(cc, ch, n).wait_send()
    for cc, ch, n in near:
        kv_copy(ch, n).wait_send()
    for ch in range(heads):
        kv_forward(ch).wait_send()
        meta_forward(ch).wait_send()

    def drain(t, carry):
        cc, ch = place_of(t)

        def finish():
            o_copy(cc, ch, t).wait_send()
            s_copy(cc, ch, t).wait_send()

        pl.when(index(cc, ch, core) != me)(finish)
        return carry

    lax.fori_loop(0, cells * heads, drain, 0)


def solution(mesh):
    members = mesh.shape["blk"]

    def shards(queries, keys, values, group_table, doc_ids):
        rows, cols = queries.shape
        group = rows // 2
        heads = cols // HEAD_DIM
        cells = members // (heads * CORES)
        doc_rows = doc_ids.reshape(-1, group)
        vmem = pl.BlockSpec(memory_space=pltpu.VMEM)
        bf16, f32 = jnp.bfloat16, jnp.float32
        dma = pltpu.SemaphoreType.DMA
        return pl.pallas_call(
            functools.partial(attend_kernel, cells),
            out_shape=jax.ShapeDtypeStruct((rows, cols), bf16),
            in_specs=[pl.BlockSpec(memory_space=pltpu.SMEM)] + [pl.BlockSpec(memory_space=pl.ANY)] * 3 + [vmem],
            out_specs=vmem,
            scratch_shapes=[
                pltpu.VMEM((heads, rows, HEAD_DIM), bf16),
                pltpu.VMEM((heads, rows, 2 * HEAD_DIM), bf16),
                pltpu.VMEM((cells, heads, rows, HEAD_DIM), bf16),
                pltpu.VMEM((heads * CORES, rows, 2 * HEAD_DIM), bf16),
                pltpu.VMEM((members, 4, group), jnp.int32),
                pltpu.VMEM((cells * heads, rows, HEAD_DIM), bf16),
                pltpu.VMEM((cells * heads, 4, group), f32),
                pltpu.VMEM((cells, heads, rows, HEAD_DIM), bf16),
                pltpu.VMEM((cells, heads, 4, group), f32),
                dma((heads,)),
                dma((heads, 2)),
                dma((3,)),
                dma((cells * heads,)),
                dma((cells, heads)),
                dma((heads,)),
                dma((heads * CORES,)),
                dma((heads,)),
                dma((cells * heads,)),
                dma((members,)),
                dma((heads,)),
                dma((cells * heads,)),
                dma((cells, heads)),
                dma((cells * heads,)),
                dma((cells, heads)),
            ],
            compiler_params=pltpu.CompilerParams(
                collective_id=0, has_side_effects=True, vmem_limit_bytes=60 * 1024 * 1024
            ),
        )(group_table, queries, keys, values, doc_rows)

    in_specs = (P("blk", "head"), P("blk", "head"), P("blk", "head"), P("blk", None), P())
    return jax.shard_map(shards, mesh=mesh, in_specs=in_specs, out_specs=P("blk", "head"), check_vma=False)
```

```python
import functools
import math

import jax
import jax.numpy as jnp
from jax import lax
from jax.experimental import pallas as pl
from jax.experimental.pallas import tpu as pltpu
from jax.sharding import PartitionSpec as P

HEAD_DIM = 128
CORES = 2
MASKED = -1e30


def attend_kernel(
    cells, table_hbm, q_hbm, k_hbm, v_hbm, doc_hbm, out_hbm,
    table_ref, doc_ref, mixed_ref, stage_q, stage_kv, qin, kv, meta, osend, ssend, obuf, sbuf,
    small_sem, out_sem, load_q, load_kv, own_sem, q_send, q_recv, kv_send, kv_recv, fwd_send, m_send, m_recv, mf_send,
    o_send, o_recv, s_send, s_recv,
):
    rows, cols = q_hbm.shape
    heads = cols // HEAD_DIM
    group = rows // 2
    factor = math.log2(math.e) / math.sqrt(HEAD_DIM)
    me = lax.axis_index("blk")
    core = lax.rem(me, CORES)
    chip = lax.rem(me // CORES, heads)
    cell = me // (CORES * heads)

    def index(cc, ch, co):
        return (cc * heads + ch) * CORES + co

    partner = index(cell, chip, 1 - core)

    def head_columns(h):
        start = h * HEAD_DIM
        if not isinstance(h, int):
            start = pl.multiple_of(start, HEAD_DIM)
        return pl.ds(start, HEAD_DIM)

    def own_slot(ch, co):
        return ch * CORES + co

    q_loads = [pltpu.make_async_copy(q_hbm.at[:, head_columns(h)], stage_q.at[h], load_q.at[h]) for h in range(heads)]
    kv_loads = []
    for h in range(heads):
        kv_loads.append((
            pltpu.make_async_copy(k_hbm.at[:, head_columns(h)], stage_kv.at[h, :, pl.ds(0, HEAD_DIM)], load_kv.at[h, 0]),
            pltpu.make_async_copy(v_hbm.at[:, head_columns(h)], stage_kv.at[h, :, pl.ds(HEAD_DIM, HEAD_DIM)], load_kv.at[h, 1]),
        ))
    own_kv = (
        pltpu.make_async_copy(k_hbm.at[:, head_columns(chip)], kv.at[own_slot(chip, core), :, pl.ds(0, HEAD_DIM)], own_sem.at[0]),
        pltpu.make_async_copy(v_hbm.at[:, head_columns(chip)], kv.at[own_slot(chip, core), :, pl.ds(HEAD_DIM, HEAD_DIM)], own_sem.at[1]),
    )
    own_q = pltpu.make_async_copy(q_hbm.at[:, head_columns(chip)], qin.at[cell, chip], own_sem.at[2])
    small_loads = (
        pltpu.make_async_copy(table_hbm, table_ref, small_sem.at[0]),
        pltpu.make_async_copy(doc_hbm, doc_ref, small_sem.at[1]),
    )
    for one in small_loads:
        one.start()
    for pair in kv_loads:
        for one in pair:
            one.start()
    for one in own_kv:
        one.start()
    for one in q_loads:
        one.start()
    own_q.start()

    barrier = pltpu.get_barrier_semaphore()
    peers = []
    for k in range(cells):
        for i in range(heads):
            if k or i:
                peers.append((lax.rem(cell + k, cells), lax.rem(chip + i, heads), k * heads + i))
    for cc, ch, _ in peers:
        pl.semaphore_signal(barrier, inc=1, device_id={"blk": index(cc, ch, core)})
    pl.semaphore_signal(barrier, inc=1, device_id={"blk": partner})

    for one in small_loads:
        one.wait()
    within = lax.broadcasted_iota(jnp.int32, (1, group), 1)
    for g in range(2):
        own_group = table_ref[0, g]
        meta[me, pl.ds(g, 1), :] = doc_ref[pl.ds(own_group, 1), :]
        meta[me, pl.ds(2 + g, 1), :] = own_group * group + within
    pl.semaphore_wait(barrier, len(peers) + 1)

    def remote(src, dst, ssem, rsem, target):
        return pltpu.make_async_remote_copy(
            src_ref=src, dst_ref=dst, send_sem=ssem, recv_sem=rsem, device_id={"blk": target}
        )

    def q_copy(cc, ch, n):
        return remote(stage_q.at[ch], qin.at[cell, chip], q_send.at[n], q_recv.at[cell, chip], index(cc, ch, core))

    def kv_copy(ch, n):
        place = own_slot(chip, core)
        return remote(stage_kv.at[ch], kv.at[place], kv_send.at[n], kv_recv.at[place], index(cell, ch, core))

    def kv_forward(ch):
        place = own_slot(ch, core)
        return remote(kv.at[place], kv.at[place], fwd_send.at[ch], kv_recv.at[place], partner)

    def meta_copy(cc, ch, n):
        return remote(meta.at[me], meta.at[me], m_send.at[n], m_recv.at[me], index(cc, ch, core))

    def meta_forward(ch):
        source = index(cell, ch, core)
        return remote(meta.at[source], meta.at[source], mf_send.at[ch], m_recv.at[source], partner)

    def q_arrival(cc, ch):
        return remote(stage_q.at[0], qin.at[cc, ch], q_send.at[0], q_recv.at[cc, ch], partner)

    def kv_arrival(place):
        return remote(kv.at[place], kv.at[place], fwd_send.at[0], kv_recv.at[place], partner)

    def meta_arrival(source):
        return remote(meta.at[source], meta.at[source], mf_send.at[0], m_recv.at[source], partner)

    near = [one for one in peers if one[2] < heads]
    far = [one for one in peers if one[2] >= heads]
    for pair in kv_loads:
        for one in pair:
            one.wait()
    for cc, ch, n in near:
        kv_copy(ch, n).start()
    for cc, ch, n in peers:
        meta_copy(cc, ch, n).start()
    meta_forward(chip).start()
    for one in own_kv:
        one.wait()
    kv_forward(chip).start()
    for one in q_loads:
        one.wait()
    for cc, ch, n in far:
        q_copy(cc, ch, n).start()
    for cc, ch, n in near:
        q_copy(cc, ch, n).start()
    own_q.wait()
    for cc, ch, n in near:
        kv_arrival(own_slot(ch, core)).wait_recv()
        kv_forward(ch).start()
        meta_arrival(index(cell, ch, core)).wait_recv()
        meta_forward(ch).start()
    for i in range(heads):
        ch = lax.rem(chip + i, heads)
        kv_arrival(own_slot(ch, 1 - core)).wait_recv()
        meta_arrival(index(cell, ch, 1 - core)).wait_recv()

    sources = heads * CORES
    key_doc = [[meta[cell * sources + s, pl.ds(g, 1), :] for s in range(sources)] for g in range(2)]
    key_pos = [[meta[cell * sources + s, pl.ds(2 + g, 1), :] for s in range(sources)] for g in range(2)]
    down = lax.broadcasted_iota(jnp.int32, (group, group), 0)
    right = lax.broadcasted_iota(jnp.int32, (group, group), 1)
    diagonal = down == right

    def to_rows(line):
        return jnp.sum(jnp.where(diagonal, line, 0), axis=1, keepdims=True)

    def to_lanes(column):
        return jnp.sum(jnp.where(diagonal, column, 0), axis=0, keepdims=True)

    def attend(q, source, slot):
        doc = jnp.broadcast_to(to_rows(meta[source, pl.ds(slot, 1), :]), (group, group))
        pos = jnp.broadcast_to(to_rows(meta[source, pl.ds(2 + slot, 1), :]), (group, group))
        parts = []
        for g in range(slot + 1):
            keys = kv[:, pl.ds(g * group, group), pl.ds(0, HEAD_DIM)].reshape(sources * group, HEAD_DIM)
            scores = lax.dot_general(q, keys, (((1,), (1,)), ((), ())), preferred_element_type=jnp.float32)
            for s in range(sources):
                seen = (key_doc[g][s] == doc) & (key_pos[g][s] <= pos)
                parts.append(jnp.where(seen, scores[:, s * group:(s + 1) * group], MASKED))
        best = parts[0]
        for one in parts[1:]:
            best = jnp.maximum(best, one)
        best = jnp.broadcast_to(jnp.max(best, axis=1, keepdims=True), (group, group))
        total = None
        out = None
        for g in range(slot + 1):
            weights = [jnp.exp2((one - best) * factor) for one in parts[g * sources:(g + 1) * sources]]
            for one in weights:
                total = one if total is None else total + one
            weights = jnp.concatenate([one.astype(jnp.bfloat16) for one in weights], axis=1)
            vals = kv[:, pl.ds(g * group, group), pl.ds(HEAD_DIM, HEAD_DIM)].reshape(sources * group, HEAD_DIM)
            add = jnp.dot(weights, vals, preferred_element_type=jnp.float32)
            out = add if out is None else out + add
        total = jnp.broadcast_to(jnp.sum(total, axis=1, keepdims=True), (group, group))
        return out, to_lanes(best), to_lanes(total)

    def o_copy(cc, ch, n):
        return remote(osend.at[n], obuf.at[cell, chip], o_send.at[n], o_recv.at[cell, chip], index(cc, ch, core))

    def s_copy(cc, ch, n):
        return remote(ssend.at[n], sbuf.at[cell, chip], s_send.at[n], s_recv.at[cell, chip], index(cc, ch, core))

    def o_arrival(cc, h):
        return remote(osend.at[0], obuf.at[cc, h], o_send.at[0], o_recv.at[cc, h], partner)

    def s_arrival(cc, h):
        return remote(ssend.at[0], sbuf.at[cc, h], s_send.at[0], s_recv.at[cc, h], partner)

    def place_of(t):
        return lax.rem(cell + 1 + t // heads, cells), lax.rem(chip + lax.rem(t, heads), heads)

    def serve(t, carry):
        cc, ch = place_of(t)
        home = index(cc, ch, core)
        other = home != me

        def arrive():
            q_arrival(cc, ch).wait_recv()

        pl.when(other)(arrive)

        def arrive_meta():
            meta_arrival(home).wait_recv()

        pl.when(cc != cell)(arrive_meta)
        for slot in range(2):
            q = qin[cc, ch, pl.ds(slot * group, group), :]
            out, best, total = attend(q, home, slot)
            osend[t, pl.ds(slot * group, group), :] = out.astype(jnp.bfloat16)
            ssend[t, pl.ds(slot, 1), :] = best
            ssend[t, pl.ds(2 + slot, 1), :] = total

        def give():
            o_copy(cc, ch, t).start()
            s_copy(cc, ch, t).start()

        pl.when(other)(give)
        return carry

    lax.fori_loop(0, cells * heads, serve, 0)

    own_turn = (cells - 1) * heads
    obuf[cell, chip] = osend[own_turn]
    sbuf[cell, chip] = ssend[own_turn]

    def out_copy(h):
        return pltpu.make_async_copy(mixed_ref.at[h], out_hbm.at[:, head_columns(h)], out_sem.at[h])

    for h in range(heads):
        for cc in range(cells):
            def arrive_partial():
                o_arrival(cc, h).wait_recv()
                s_arrival(cc, h).wait_recv()

            pl.when((cell != cc) | (chip != h))(arrive_partial)
        for slot in range(2):
            part = pl.ds(slot * group, group)
            tops = [sbuf[cc, h, pl.ds(slot, 1), :] for cc in range(cells)]
            sums = [sbuf[cc, h, pl.ds(2 + slot, 1), :] for cc in range(cells)]
            top = functools.reduce(jnp.maximum, tops)
            scale = [jnp.exp2((one - top) * factor) for one in tops]
            total = functools.reduce(jnp.add, [a * b for a, b in zip(scale, sums)])
            mixed = None
            for cc in range(cells):
                weight = to_rows(scale[cc] / total)
                term = obuf[cc, h, part, :].astype(jnp.float32) * weight
                mixed = term if mixed is None else mixed + term
            mixed_ref[h, part, :] = mixed.astype(mixed_ref.dtype)
        out_copy(h).start()

    for cc, ch, n in peers:
        q_copy(cc, ch, n).wait_send()
        meta_copy(cc, ch, n).wait_send()
    for cc, ch, n in near:
        kv_copy(ch, n).wait_send()
    for ch in range(heads):
        kv_forward(ch).wait_send()
        meta_forward(ch).wait_send()

    def drain(t, carry):
        cc, ch = place_of(t)

        def finish():
            o_copy(cc, ch, t).wait_send()
            s_copy(cc, ch, t).wait_send()

        pl.when(index(cc, ch, core) != me)(finish)
        return carry

    lax.fori_loop(0, cells * heads, drain, 0)
    for h in range(heads):
        out_copy(h).wait()


def solution(mesh):
    members = mesh.shape["blk"]

    def shards(queries, keys, values, group_table, doc_ids):
        rows, cols = queries.shape
        group = rows // 2
        heads = cols // HEAD_DIM
        cells = members // (heads * CORES)
        doc_rows = doc_ids.reshape(-1, group)
        bf16, f32 = jnp.bfloat16, jnp.float32
        dma = pltpu.SemaphoreType.DMA
        return pl.pallas_call(
            functools.partial(attend_kernel, cells),
            out_shape=jax.ShapeDtypeStruct((rows, cols), bf16),
            in_specs=[pl.BlockSpec(memory_space=pl.ANY)] * 5,
            out_specs=pl.BlockSpec(memory_space=pl.ANY),
            scratch_shapes=[
                pltpu.SMEM((1, 2), jnp.int32),
                pltpu.VMEM(doc_rows.shape, jnp.int32),
                pltpu.VMEM((heads, rows, HEAD_DIM), bf16),
                pltpu.VMEM((heads, rows, HEAD_DIM), bf16),
                pltpu.VMEM((heads, rows, 2 * HEAD_DIM), bf16),
                pltpu.VMEM((cells, heads, rows, HEAD_DIM), bf16),
                pltpu.VMEM((heads * CORES, rows, 2 * HEAD_DIM), bf16),
                pltpu.VMEM((members, 4, group), jnp.int32),
                pltpu.VMEM((cells * heads, rows, HEAD_DIM), bf16),
                pltpu.VMEM((cells * heads, 4, group), f32),
                pltpu.VMEM((cells, heads, rows, HEAD_DIM), bf16),
                pltpu.VMEM((cells, heads, 4, group), f32),
                dma((2,)),
                dma((heads,)),
                dma((heads,)),
                dma((heads, 2)),
                dma((3,)),
                dma((cells * heads,)),
                dma((cells, heads)),
                dma((heads,)),
                dma((heads * CORES,)),
                dma((heads,)),
                dma((cells * heads,)),
                dma((members,)),
                dma((heads,)),
                dma((cells * heads,)),
                dma((cells, heads)),
                dma((cells * heads,)),
                dma((cells, heads)),
            ],
            compiler_params=pltpu.CompilerParams(
                collective_id=0, has_side_effects=True, vmem_limit_bytes=60 * 1024 * 1024
            ),
        )(group_table, queries, keys, values, doc_rows)

    in_specs = (P("blk", "head"), P("blk", "head"), P("blk", "head"), P("blk", None), P())
    return jax.shard_map(shards, mesh=mesh, in_specs=in_specs, out_specs=P("blk", "head"), check_vma=False)
```

```python
import functools
import math

import jax
import jax.numpy as jnp
from jax import lax
from jax.experimental import pallas as pl
from jax.experimental.pallas import tpu as pltpu
from jax.sharding import PartitionSpec as P

HEAD_DIM = 128
CORES = 2
MASKED = -1e30


def attend_kernel(
    cells, table_hbm, q_hbm, k_hbm, v_hbm, doc_hbm, out_hbm,
    table_ref, doc_ref, mixed_ref, stage_q, stage_kv, qin, kv, meta, osend, ssend, obuf, sbuf,
    small_sem, out_sem, load_q, load_kv, own_sem, q_send, q_recv, kv_send, kv_recv, fwd_send, m_send, m_recv, mf_send,
    o_send, o_recv, s_send, s_recv,
):
    rows, cols = q_hbm.shape
    heads = cols // HEAD_DIM
    group = rows // 2
    factor = math.log2(math.e) / math.sqrt(HEAD_DIM)
    me = lax.axis_index("blk")
    core = lax.rem(me, CORES)
    chip = lax.rem(me // CORES, heads)
    cell = me // (CORES * heads)

    def index(cc, ch, co):
        return (cc * heads + ch) * CORES + co

    partner = index(cell, chip, 1 - core)

    def facing(other, i):
        return lax.rem(i + (heads // 2) * (other < cell).astype(jnp.int32), heads)

    def head_columns(h):
        start = h * HEAD_DIM
        if not isinstance(h, int):
            start = pl.multiple_of(start, HEAD_DIM)
        return pl.ds(start, HEAD_DIM)

    def own_slot(ch, co):
        return ch * CORES + co

    q_loads = [pltpu.make_async_copy(q_hbm.at[:, head_columns(h)], stage_q.at[h], load_q.at[h]) for h in range(heads)]
    kv_loads = []
    for h in range(heads):
        kv_loads.append((
            pltpu.make_async_copy(k_hbm.at[:, head_columns(h)], stage_kv.at[h, :, pl.ds(0, HEAD_DIM)], load_kv.at[h, 0]),
            pltpu.make_async_copy(v_hbm.at[:, head_columns(h)], stage_kv.at[h, :, pl.ds(HEAD_DIM, HEAD_DIM)], load_kv.at[h, 1]),
        ))
    own_kv = (
        pltpu.make_async_copy(k_hbm.at[:, head_columns(chip)], kv.at[own_slot(chip, core), :, pl.ds(0, HEAD_DIM)], own_sem.at[0]),
        pltpu.make_async_copy(v_hbm.at[:, head_columns(chip)], kv.at[own_slot(chip, core), :, pl.ds(HEAD_DIM, HEAD_DIM)], own_sem.at[1]),
    )
    own_q = pltpu.make_async_copy(q_hbm.at[:, head_columns(chip)], qin.at[cell, chip], own_sem.at[2])
    small_loads = (
        pltpu.make_async_copy(table_hbm, table_ref, small_sem.at[0]),
        pltpu.make_async_copy(doc_hbm, doc_ref, small_sem.at[1]),
    )
    for one in small_loads:
        one.start()
    for pair in kv_loads:
        for one in pair:
            one.start()
    for one in own_kv:
        one.start()
    for one in q_loads:
        one.start()
    own_q.start()

    barrier = pltpu.get_barrier_semaphore()
    peers = []
    for i in range(heads - 1, 0, -1):
        peers.append((cell, chip ^ i, i))
    for k in range(1, cells):
        other = lax.rem(cell + k, cells)
        for i in range(heads):
            peers.append((other, facing(other, i) ^ lax.rem(chip, 2), k * heads + i))
    for cc, ch, _ in peers:
        pl.semaphore_signal(barrier, inc=1, device_id={"blk": index(cc, ch, core)})
    pl.semaphore_signal(barrier, inc=1, device_id={"blk": partner})

    for one in small_loads:
        one.wait()
    within = lax.broadcasted_iota(jnp.int32, (1, group), 1)
    for g in range(2):
        own_group = table_ref[0, g]
        meta[me, pl.ds(g, 1), :] = doc_ref[pl.ds(own_group, 1), :].astype(jnp.float32)
        meta[me, pl.ds(2 + g, 1), :] = (own_group * group + within).astype(jnp.float32)
    pl.semaphore_wait(barrier, len(peers) + 1)

    def remote(src, dst, ssem, rsem, target):
        return pltpu.make_async_remote_copy(
            src_ref=src, dst_ref=dst, send_sem=ssem, recv_sem=rsem, device_id={"blk": target}
        )

    def q_copy(cc, ch, n):
        return remote(stage_q.at[ch], qin.at[cell, chip], q_send.at[n], q_recv.at[cell, chip], index(cc, ch, core))

    def kv_copy(ch, n):
        place = own_slot(chip, core)
        return remote(stage_kv.at[ch], kv.at[place], kv_send.at[n], kv_recv.at[place], index(cell, ch, core))

    def kv_forward(ch):
        place = own_slot(ch, core)
        return remote(kv.at[place], kv.at[place], fwd_send.at[ch], kv_recv.at[place], partner)

    def meta_copy(cc, ch, n):
        return remote(meta.at[me], meta.at[me], m_send.at[n], m_recv.at[me], index(cc, ch, core))

    def meta_forward(ch):
        source = index(cell, ch, core)
        return remote(meta.at[source], meta.at[source], mf_send.at[ch], m_recv.at[source], partner)

    def q_arrival(cc, ch):
        return remote(stage_q.at[0], qin.at[cc, ch], q_send.at[0], q_recv.at[cc, ch], partner)

    def kv_arrival(place):
        return remote(kv.at[place], kv.at[place], fwd_send.at[0], kv_recv.at[place], partner)

    def meta_arrival(source):
        return remote(meta.at[source], meta.at[source], mf_send.at[0], m_recv.at[source], partner)

    near = [one for one in peers if one[2] < heads]
    far = [one for one in peers if one[2] >= heads]
    for cc, ch, n in peers:
        meta_copy(cc, ch, n).start()
    meta_forward(chip).start()
    for pair in kv_loads:
        for one in pair:
            one.wait()
    for cc, ch, n in near:
        kv_copy(ch, n).start()
    for one in own_kv:
        one.wait()
    kv_forward(chip).start()
    for one in q_loads:
        one.wait()
    for cc, ch, n in far:
        q_copy(cc, ch, n).start()
    for cc, ch, n in near:
        q_copy(cc, ch, n).start()
    own_q.wait()
    for cc, ch, n in near:
        kv_arrival(own_slot(ch, core)).wait_recv()
        kv_forward(ch).start()
        meta_arrival(index(cell, ch, core)).wait_recv()
        meta_forward(ch).start()
    for i in range(heads):
        ch = lax.rem(chip + i, heads)
        kv_arrival(own_slot(ch, 1 - core)).wait_recv()
        meta_arrival(index(cell, ch, 1 - core)).wait_recv()

    sources = heads * CORES
    down = lax.broadcasted_iota(jnp.int32, (group, group), 0)
    right = lax.broadcasted_iota(jnp.int32, (group, group), 1)
    diagonal = down == right

    def to_rows(line):
        return jnp.sum(jnp.where(diagonal, line, 0.0), axis=1, keepdims=True)

    def to_lanes(column):
        return jnp.sum(jnp.where(diagonal, column, 0.0), axis=0, keepdims=True)

    def attend(cc, ch, home):
        order = [lax.rem(own_slot(ch, core) + i, sources) for i in range(sources)]
        q = qin[cc, ch]
        doc_line = [meta[home, pl.ds(slot, 1), :] for slot in range(2)]
        pos_line = [meta[home, pl.ds(2 + slot, 1), :] for slot in range(2)]
        doc = [jnp.broadcast_to(to_rows(one), (group, group)) for one in doc_line]
        pos = [jnp.broadcast_to(to_rows(one), (group, group)) for one in pos_line]
        parts = [[], []]
        for g in range(2):
            part = pl.ds(g * group, group)
            keys = jnp.concatenate([kv[s, part, pl.ds(0, HEAD_DIM)] for s in order], axis=0)
            scores = lax.dot_general(
                q if g == 0 else q[group:], keys, (((1,), (1,)), ((), ())), preferred_element_type=jnp.float32
            )
            for i, s in enumerate(order):
                key_doc = meta[cell * sources + s, pl.ds(g, 1), :]
                key_pos = meta[cell * sources + s, pl.ds(2 + g, 1), :]
                for slot in range(g, 2):
                    row = (slot - g) * group
                    block = scores[row:row + group, i * group:(i + 1) * group]
                    if i:
                        seen = jnp.where(key_pos < pos_line[slot], key_doc, -1.0) == doc[slot]
                    else:
                        seen = (key_doc == doc[slot]) & (key_pos <= pos[slot])
                    parts[slot].append(jnp.where(seen, block, MASKED))
        best = []
        weights = []
        sums = []
        for slot in range(2):
            top = functools.reduce(jnp.maximum, parts[slot])
            top = jnp.broadcast_to(jnp.max(top, axis=1, keepdims=True), (group, group))
            found = [jnp.exp2((one - top) * factor) for one in parts[slot]]
            total = jnp.sum(functools.reduce(jnp.add, found), axis=1, keepdims=True)
            best.append(to_lanes(top))
            sums.append(to_lanes(jnp.broadcast_to(total, (group, group))))
            weights.append([one.astype(jnp.bfloat16) for one in found])
        outs = []
        for g in range(2):
            part = pl.ds(g * group, group)
            vals = jnp.concatenate([kv[s, part, pl.ds(HEAD_DIM, HEAD_DIM)] for s in order], axis=0)
            lines = [jnp.concatenate(weights[slot][g * sources:(g + 1) * sources], axis=1) for slot in range(g, 2)]
            line = lines[0] if g else jnp.concatenate(lines, axis=0)
            outs.append(jnp.dot(line, vals, preferred_element_type=jnp.float32))
        return (outs[0][:group], outs[0][group:] + outs[1]), best, sums

    def o_copy(cc, ch, n):
        return remote(osend.at[n], obuf.at[cell, chip], o_send.at[n], o_recv.at[cell, chip], index(cc, ch, core))

    def s_copy(cc, ch, n):
        return remote(ssend.at[n], sbuf.at[cell, chip], s_send.at[n], s_recv.at[cell, chip], index(cc, ch, core))

    def o_arrival(cc, h):
        return remote(osend.at[0], obuf.at[cc, h], o_send.at[0], o_recv.at[cc, h], partner)

    def s_arrival(cc, h):
        return remote(ssend.at[0], sbuf.at[cc, h], s_send.at[0], s_recv.at[cc, h], partner)

    def place_of(t):
        cc = lax.rem(cell + 1 + t // heads, cells)
        return cc, facing(cc, lax.rem(t, heads))

    def serve(t, carry):
        cc, ch = place_of(t)
        home = index(cc, ch, core)
        other = home != me

        def arrive():
            q_arrival(cc, ch).wait_recv()

        pl.when(other)(arrive)

        def arrive_meta():
            meta_arrival(home).wait_recv()

        pl.when(cc != cell)(arrive_meta)
        outs, best, sums = attend(cc, ch, home)
        for slot in range(2):
            osend[t, pl.ds(slot * group, group), :] = outs[slot].astype(jnp.bfloat16)
            ssend[t, pl.ds(slot, 1), :] = best[slot]
            ssend[t, pl.ds(2 + slot, 1), :] = sums[slot]

        def give():
            o_copy(cc, ch, t).start()
            s_copy(cc, ch, t).start()

        pl.when(other)(give)
        return carry

    lax.fori_loop(0, cells * heads, serve, 0)

    own_turn = (cells - 1) * heads + chip
    obuf[cell, chip] = osend[own_turn]
    sbuf[cell, chip] = ssend[own_turn]

    def out_copy(h):
        return pltpu.make_async_copy(mixed_ref.at[h], out_hbm.at[:, head_columns(h)], out_sem.at[h])

    for h in range(heads):
        for cc in range(cells):
            def arrive_partial():
                o_arrival(cc, h).wait_recv()
                s_arrival(cc, h).wait_recv()

            pl.when((cell != cc) | (chip != h))(arrive_partial)
        for slot in range(2):
            part = pl.ds(slot * group, group)
            tops = [sbuf[cc, h, pl.ds(slot, 1), :] for cc in range(cells)]
            sums = [sbuf[cc, h, pl.ds(2 + slot, 1), :] for cc in range(cells)]
            top = functools.reduce(jnp.maximum, tops)
            scale = [jnp.exp2((one - top) * factor) for one in tops]
            total = functools.reduce(jnp.add, [a * b for a, b in zip(scale, sums)])
            mixed = None
            for cc in range(cells):
                weight = to_rows(scale[cc] / total)
                term = obuf[cc, h, part, :].astype(jnp.float32) * weight
                mixed = term if mixed is None else mixed + term
            out_hbm[part, pl.ds(h * HEAD_DIM, HEAD_DIM)] = mixed.astype(out_hbm.dtype)

    for cc, ch, n in peers:
        q_copy(cc, ch, n).wait_send()
        meta_copy(cc, ch, n).wait_send()
    for cc, ch, n in near:
        kv_copy(ch, n).wait_send()
    for ch in range(heads):
        kv_forward(ch).wait_send()
        meta_forward(ch).wait_send()

    def drain(t, carry):
        cc, ch = place_of(t)

        def finish():
            o_copy(cc, ch, t).wait_send()
            s_copy(cc, ch, t).wait_send()

        pl.when(index(cc, ch, core) != me)(finish)
        return carry

    lax.fori_loop(0, cells * heads, drain, 0)


def solution(mesh):
    members = mesh.shape["blk"]

    def shards(queries, keys, values, group_table, doc_ids):
        rows, cols = queries.shape
        group = rows // 2
        heads = cols // HEAD_DIM
        cells = members // (heads * CORES)
        doc_rows = doc_ids.reshape(-1, group)
        bf16, f32 = jnp.bfloat16, jnp.float32
        dma = pltpu.SemaphoreType.DMA
        return pl.pallas_call(
            functools.partial(attend_kernel, cells),
            out_shape=jax.ShapeDtypeStruct((rows, cols), bf16),
            in_specs=[pl.BlockSpec(memory_space=pl.ANY)] * 5,
            out_specs=pl.BlockSpec(memory_space=pltpu.VMEM),
            scratch_shapes=[
                pltpu.SMEM((1, 2), jnp.int32),
                pltpu.VMEM(doc_rows.shape, jnp.int32),
                pltpu.VMEM((heads, rows, HEAD_DIM), bf16),
                pltpu.VMEM((heads, rows, HEAD_DIM), bf16),
                pltpu.VMEM((heads, rows, 2 * HEAD_DIM), bf16),
                pltpu.VMEM((cells, heads, rows, HEAD_DIM), bf16),
                pltpu.VMEM((heads * CORES, rows, 2 * HEAD_DIM), bf16),
                pltpu.VMEM((members, 4, group), f32),
                pltpu.VMEM((cells * heads, rows, HEAD_DIM), bf16),
                pltpu.VMEM((cells * heads, 4, group), f32),
                pltpu.VMEM((cells, heads, rows, HEAD_DIM), bf16),
                pltpu.VMEM((cells, heads, 4, group), f32),
                dma((2,)),
                dma((heads,)),
                dma((heads,)),
                dma((heads, 2)),
                dma((3,)),
                dma((cells * heads,)),
                dma((cells, heads)),
                dma((heads,)),
                dma((heads * CORES,)),
                dma((heads,)),
                dma((cells * heads,)),
                dma((members,)),
                dma((heads,)),
                dma((cells * heads,)),
                dma((cells, heads)),
                dma((cells * heads,)),
                dma((cells, heads)),
            ],
            compiler_params=pltpu.CompilerParams(
                collective_id=0, has_side_effects=True, vmem_limit_bytes=12 * 1024 * 1024
            ),
        )(*[pltpu.with_memory_space_constraint(one, pltpu.HBM) for one in (group_table, queries, keys, values, doc_rows)])

    in_specs = (P("blk", "head"), P("blk", "head"), P("blk", "head"), P("blk", None), P())
    return jax.shard_map(shards, mesh=mesh, in_specs=in_specs, out_specs=P("blk", "head"), check_vma=False)
```

```python
import functools
import math

import jax
import jax.numpy as jnp
from jax import lax
from jax.experimental import pallas as pl
from jax.experimental.pallas import tpu as pltpu
from jax.sharding import PartitionSpec as P

HEAD_DIM = 128
CORES = 2
MASKED = -1e30


def attend_kernel(
    cells, table_hbm, q_hbm, k_hbm, v_hbm, doc_hbm, out_hbm,
    table_ref, doc_ref, mixed_ref, stage_q, stage_kv, qin, kv, meta, osend, ssend, obuf, sbuf,
    ready, small_sem, out_sem, load_q, load_kv, own_sem, q_send, q_recv, kv_send, kv_recv, fwd_send, m_send, m_recv, mf_send,
    o_send, o_recv, s_send, s_recv,
):
    rows, cols = q_hbm.shape
    heads = cols // HEAD_DIM
    group = rows // 2
    factor = math.log2(math.e) / math.sqrt(HEAD_DIM)
    me = lax.axis_index("blk")
    core = lax.rem(me, CORES)
    chip = lax.rem(me // CORES, heads)
    cell = me // (CORES * heads)

    def index(cc, ch, co):
        return (cc * heads + ch) * CORES + co

    partner = index(cell, chip, 1 - core)

    def facing(other, i):
        return lax.rem(i + (heads // 2) * (other < cell).astype(jnp.int32), heads)

    def head_columns(h):
        start = h * HEAD_DIM
        if not isinstance(h, int):
            start = pl.multiple_of(start, HEAD_DIM)
        return pl.ds(start, HEAD_DIM)

    def own_slot(ch, co):
        return ch * CORES + co

    q_loads = [pltpu.make_async_copy(q_hbm.at[:, head_columns(h)], stage_q.at[h], load_q.at[h]) for h in range(heads)]
    kv_loads = []
    for h in range(heads):
        kv_loads.append((
            pltpu.make_async_copy(k_hbm.at[:, head_columns(h)], stage_kv.at[h, :, pl.ds(0, HEAD_DIM)], load_kv.at[h, 0]),
            pltpu.make_async_copy(v_hbm.at[:, head_columns(h)], stage_kv.at[h, :, pl.ds(HEAD_DIM, HEAD_DIM)], load_kv.at[h, 1]),
        ))
    own_kv = (
        pltpu.make_async_copy(k_hbm.at[:, head_columns(chip)], kv.at[own_slot(chip, core), :, pl.ds(0, HEAD_DIM)], own_sem.at[0]),
        pltpu.make_async_copy(v_hbm.at[:, head_columns(chip)], kv.at[own_slot(chip, core), :, pl.ds(HEAD_DIM, HEAD_DIM)], own_sem.at[1]),
    )
    own_q = pltpu.make_async_copy(q_hbm.at[:, head_columns(chip)], qin.at[cell, chip], own_sem.at[2])
    small_loads = (
        pltpu.make_async_copy(table_hbm, table_ref, small_sem.at[0]),
        pltpu.make_async_copy(doc_hbm, doc_ref, small_sem.at[1]),
    )
    for one in small_loads:
        one.start()
    for pair in kv_loads:
        for one in pair:
            one.start()
    for one in own_kv:
        one.start()
    for one in q_loads:
        one.start()
    own_q.start()

    barrier = pltpu.get_barrier_semaphore()
    peers = []
    for i in range(heads - 1, 0, -1):
        peers.append((cell, chip ^ i, i))
    for k in range(1, cells):
        other = lax.rem(cell + k, cells)
        for i in range(heads):
            peers.append((other, facing(other, i) ^ lax.rem(chip, 2), k * heads + i))
    mates = [one for one in peers if one[2] < heads]
    others = [one for one in peers if one[2] >= heads]
    for cc, ch, _ in mates:
        pl.semaphore_signal(barrier, inc=1, device_id={"blk": index(cc, ch, 0)})
    for cc, ch, _ in others:
        pl.semaphore_signal(barrier, inc=1, device_id={"blk": index(cc, ch, 1)})

    def greet_partner():
        pl.semaphore_signal(barrier, inc=1, device_id={"blk": partner})

    pl.when(core == 1)(greet_partner)

    def cell_here():
        def hear():
            pl.semaphore_wait(barrier, CORES * len(mates) + 1)
            pl.semaphore_signal(ready.at[0], inc=1, device_id={"blk": partner})

        pl.when(core == 0)(hear)
        pl.when(core == 1)(lambda: pl.semaphore_wait(ready.at[0], 1))

    def others_here():
        def hear():
            pl.semaphore_wait(barrier, CORES * len(others))
            pl.semaphore_signal(ready.at[1], inc=1, device_id={"blk": partner})

        pl.when(core == 1)(hear)
        pl.when(core == 0)(lambda: pl.semaphore_wait(ready.at[1], 1))

    for one in small_loads:
        one.wait()
    within = lax.broadcasted_iota(jnp.int32, (1, group), 1)
    for g in range(2):
        own_group = table_ref[0, g]
        meta[me, pl.ds(g, 1), :] = doc_ref[pl.ds(own_group, 1), :].astype(jnp.float32)
        meta[me, pl.ds(2 + g, 1), :] = (own_group * group + within).astype(jnp.float32)
    cell_here()

    def remote(src, dst, ssem, rsem, target):
        return pltpu.make_async_remote_copy(
            src_ref=src, dst_ref=dst, send_sem=ssem, recv_sem=rsem, device_id={"blk": target}
        )

    def q_copy(cc, ch, n):
        return remote(stage_q.at[ch], qin.at[cell, chip], q_send.at[n], q_recv.at[cell, chip], index(cc, ch, core))

    def kv_copy(ch, n):
        place = own_slot(chip, core)
        return remote(stage_kv.at[ch], kv.at[place], kv_send.at[n], kv_recv.at[place], index(cell, ch, core))

    def kv_forward(ch):
        place = own_slot(ch, core)
        return remote(kv.at[place], kv.at[place], fwd_send.at[ch], kv_recv.at[place], partner)

    def meta_copy(cc, ch, n):
        return remote(meta.at[me], meta.at[me], m_send.at[n], m_recv.at[me], index(cc, ch, core))

    def meta_forward(ch):
        source = index(cell, ch, core)
        return remote(meta.at[source], meta.at[source], mf_send.at[ch], m_recv.at[source], partner)

    def q_arrival(cc, ch):
        return remote(stage_q.at[0], qin.at[cc, ch], q_send.at[0], q_recv.at[cc, ch], partner)

    def kv_arrival(place):
        return remote(kv.at[place], kv.at[place], fwd_send.at[0], kv_recv.at[place], partner)

    def meta_arrival(source):
        return remote(meta.at[source], meta.at[source], mf_send.at[0], m_recv.at[source], partner)

    near = [one for one in peers if one[2] < heads]
    far = [one for one in peers if one[2] >= heads]
    for cc, ch, n in near:
        meta_copy(cc, ch, n).start()
    meta_forward(chip).start()
    for pair in kv_loads:
        for one in pair:
            one.wait()
    for cc, ch, n in near:
        kv_copy(ch, n).start()
    for one in own_kv:
        one.wait()
    kv_forward(chip).start()
    for one in q_loads:
        one.wait()
    others_here()
    for cc, ch, n in far:
        meta_copy(cc, ch, n).start()
    for cc, ch, n in far:
        q_copy(cc, ch, n).start()
    for cc, ch, n in near:
        q_copy(cc, ch, n).start()
    own_q.wait()
    for cc, ch, n in near:
        kv_arrival(own_slot(ch, core)).wait_recv()
        kv_forward(ch).start()
        meta_arrival(index(cell, ch, core)).wait_recv()
        meta_forward(ch).start()
    for i in range(heads):
        ch = lax.rem(chip + i, heads)
        kv_arrival(own_slot(ch, 1 - core)).wait_recv()
        meta_arrival(index(cell, ch, 1 - core)).wait_recv()

    sources = heads * CORES
    down = lax.broadcasted_iota(jnp.int32, (group, group), 0)
    right = lax.broadcasted_iota(jnp.int32, (group, group), 1)
    diagonal = down == right

    def to_rows(line):
        return jnp.sum(jnp.where(diagonal, line, 0.0), axis=1, keepdims=True)

    def to_lanes(column):
        return jnp.sum(jnp.where(diagonal, column, 0.0), axis=0, keepdims=True)

    def attend(cc, ch, home):
        order = [lax.rem(own_slot(ch, core) + i, sources) for i in range(sources)]
        q = qin[cc, ch]
        doc_line = [meta[home, pl.ds(slot, 1), :] for slot in range(2)]
        pos_line = [meta[home, pl.ds(2 + slot, 1), :] for slot in range(2)]
        doc = [jnp.broadcast_to(to_rows(one), (group, group)) for one in doc_line]
        pos = [jnp.broadcast_to(to_rows(one), (group, group)) for one in pos_line]
        parts = [[], []]
        for g in range(2):
            part = pl.ds(g * group, group)
            keys = jnp.concatenate([kv[s, part, pl.ds(0, HEAD_DIM)] for s in order], axis=0)
            scores = lax.dot_general(
                q if g == 0 else q[group:], keys, (((1,), (1,)), ((), ())), preferred_element_type=jnp.float32
            )
            for i, s in enumerate(order):
                key_doc = meta[cell * sources + s, pl.ds(g, 1), :]
                key_pos = meta[cell * sources + s, pl.ds(2 + g, 1), :]
                for slot in range(g, 2):
                    row = (slot - g) * group
                    block = scores[row:row + group, i * group:(i + 1) * group]
                    if i:
                        seen = jnp.where(key_pos < pos_line[slot], key_doc, -1.0) == doc[slot]
                    else:
                        seen = (key_doc == doc[slot]) & (key_pos <= pos[slot])
                    parts[slot].append(jnp.where(seen, block, MASKED))
        best = []
        weights = []
        sums = []
        for slot in range(2):
            top = functools.reduce(jnp.maximum, parts[slot])
            top = jnp.broadcast_to(jnp.max(top, axis=1, keepdims=True), (group, group))
            found = [jnp.exp2((one - top) * factor) for one in parts[slot]]
            total = jnp.sum(functools.reduce(jnp.add, found), axis=1, keepdims=True)
            best.append(to_lanes(top))
            sums.append(to_lanes(jnp.broadcast_to(total, (group, group))))
            weights.append([one.astype(jnp.bfloat16) for one in found])
        outs = []
        for g in range(2):
            part = pl.ds(g * group, group)
            vals = jnp.concatenate([kv[s, part, pl.ds(HEAD_DIM, HEAD_DIM)] for s in order], axis=0)
            lines = [jnp.concatenate(weights[slot][g * sources:(g + 1) * sources], axis=1) for slot in range(g, 2)]
            line = lines[0] if g else jnp.concatenate(lines, axis=0)
            outs.append(jnp.dot(line, vals, preferred_element_type=jnp.float32))
        return (outs[0][:group], outs[0][group:] + outs[1]), best, sums

    def o_copy(cc, ch, n):
        return remote(osend.at[n], obuf.at[cell, chip], o_send.at[n], o_recv.at[cell, chip], index(cc, ch, core))

    def s_copy(cc, ch, n):
        return remote(ssend.at[n], sbuf.at[cell, chip], s_send.at[n], s_recv.at[cell, chip], index(cc, ch, core))

    def o_arrival(cc, h):
        return remote(osend.at[0], obuf.at[cc, h], o_send.at[0], o_recv.at[cc, h], partner)

    def s_arrival(cc, h):
        return remote(ssend.at[0], sbuf.at[cc, h], s_send.at[0], s_recv.at[cc, h], partner)

    def place_of(t):
        cc = lax.rem(cell + 1 + t // heads, cells)
        return cc, facing(cc, lax.rem(t, heads))

    def serve(t, carry):
        cc, ch = place_of(t)
        home = index(cc, ch, core)
        other = home != me

        def arrive():
            q_arrival(cc, ch).wait_recv()

        pl.when(other)(arrive)

        def arrive_meta():
            meta_arrival(home).wait_recv()

        pl.when(cc != cell)(arrive_meta)
        outs, best, sums = attend(cc, ch, home)
        for slot in range(2):
            osend[t, pl.ds(slot * group, group), :] = outs[slot].astype(jnp.bfloat16)
            ssend[t, pl.ds(slot, 1), :] = best[slot]
            ssend[t, pl.ds(2 + slot, 1), :] = sums[slot]

        def give():
            o_copy(cc, ch, t).start()
            s_copy(cc, ch, t).start()

        pl.when(other)(give)
        return carry

    lax.fori_loop(0, cells * heads, serve, 0)

    own_turn = (cells - 1) * heads + chip
    obuf[cell, chip] = osend[own_turn]
    sbuf[cell, chip] = ssend[own_turn]

    def out_copy(h):
        return pltpu.make_async_copy(mixed_ref.at[h], out_hbm.at[:, head_columns(h)], out_sem.at[h])

    for h in range(heads):
        for cc in range(cells):
            def arrive_partial():
                o_arrival(cc, h).wait_recv()
                s_arrival(cc, h).wait_recv()

            pl.when((cell != cc) | (chip != h))(arrive_partial)
        for slot in range(2):
            part = pl.ds(slot * group, group)
            tops = [sbuf[cc, h, pl.ds(slot, 1), :] for cc in range(cells)]
            sums = [sbuf[cc, h, pl.ds(2 + slot, 1), :] for cc in range(cells)]
            top = functools.reduce(jnp.maximum, tops)
            scale = [jnp.exp2((one - top) * factor) for one in tops]
            total = functools.reduce(jnp.add, [a * b for a, b in zip(scale, sums)])
            mixed = None
            for cc in range(cells):
                weight = to_rows(scale[cc] / total)
                term = obuf[cc, h, part, :].astype(jnp.float32) * weight
                mixed = term if mixed is None else mixed + term
            out_hbm[part, pl.ds(h * HEAD_DIM, HEAD_DIM)] = mixed.astype(out_hbm.dtype)

    for cc, ch, n in peers:
        q_copy(cc, ch, n).wait_send()
        meta_copy(cc, ch, n).wait_send()
    for cc, ch, n in near:
        kv_copy(ch, n).wait_send()
    for ch in range(heads):
        kv_forward(ch).wait_send()
        meta_forward(ch).wait_send()

    def drain(t, carry):
        cc, ch = place_of(t)

        def finish():
            o_copy(cc, ch, t).wait_send()
            s_copy(cc, ch, t).wait_send()

        pl.when(index(cc, ch, core) != me)(finish)
        return carry

    lax.fori_loop(0, cells * heads, drain, 0)


def solution(mesh):
    members = mesh.shape["blk"]

    def shards(queries, keys, values, group_table, doc_ids):
        rows, cols = queries.shape
        group = rows // 2
        heads = cols // HEAD_DIM
        cells = members // (heads * CORES)
        doc_rows = doc_ids.reshape(-1, group)
        bf16, f32 = jnp.bfloat16, jnp.float32
        dma = pltpu.SemaphoreType.DMA
        return pl.pallas_call(
            functools.partial(attend_kernel, cells),
            out_shape=jax.ShapeDtypeStruct((rows, cols), bf16),
            in_specs=[pl.BlockSpec(memory_space=pl.ANY)] * 5,
            out_specs=pl.BlockSpec(memory_space=pltpu.VMEM),
            scratch_shapes=[
                pltpu.SMEM((1, 2), jnp.int32),
                pltpu.VMEM(doc_rows.shape, jnp.int32),
                pltpu.VMEM((heads, rows, HEAD_DIM), bf16),
                pltpu.VMEM((heads, rows, HEAD_DIM), bf16),
                pltpu.VMEM((heads, rows, 2 * HEAD_DIM), bf16),
                pltpu.VMEM((cells, heads, rows, HEAD_DIM), bf16),
                pltpu.VMEM((heads * CORES, rows, 2 * HEAD_DIM), bf16),
                pltpu.VMEM((members, 4, group), f32),
                pltpu.VMEM((cells * heads, rows, HEAD_DIM), bf16),
                pltpu.VMEM((cells * heads, 4, group), f32),
                pltpu.VMEM((cells, heads, rows, HEAD_DIM), bf16),
                pltpu.VMEM((cells, heads, 4, group), f32),
                pltpu.SemaphoreType.REGULAR((2,)),
                dma((2,)),
                dma((heads,)),
                dma((heads,)),
                dma((heads, 2)),
                dma((3,)),
                dma((cells * heads,)),
                dma((cells, heads)),
                dma((heads,)),
                dma((heads * CORES,)),
                dma((heads,)),
                dma((cells * heads,)),
                dma((members,)),
                dma((heads,)),
                dma((cells * heads,)),
                dma((cells, heads)),
                dma((cells * heads,)),
                dma((cells, heads)),
            ],
            compiler_params=pltpu.CompilerParams(
                collective_id=0, has_side_effects=True, vmem_limit_bytes=12 * 1024 * 1024
            ),
        )(*[pltpu.with_memory_space_constraint(one, pltpu.HBM) for one in (group_table, queries, keys, values, doc_rows)])

    in_specs = (P("blk", "head"), P("blk", "head"), P("blk", "head"), P("blk", None), P())
    return jax.shard_map(shards, mesh=mesh, in_specs=in_specs, out_specs=P("blk", "head"), check_vma=False)
```

```python
import functools
import math

import jax
import jax.numpy as jnp
from jax import lax
from jax.experimental import pallas as pl
from jax.experimental.pallas import tpu as pltpu
from jax.sharding import PartitionSpec as P

HEAD_DIM = 128
CORES = 2
MASKED = -1e30


def attend_kernel(
    cells, table_hbm, q_hbm, k_hbm, v_hbm, doc_hbm, out_ref,
    table_ref, doc_ref, stage_q, stage_kv, qin, kv, meta, osend, ssend, obuf, sbuf, measure,
    ready, small_sem, load_q, load_kv, own_sem, q_send, q_recv, kv_send, kv_recv, fwd_send, m_send, mf_send,
    o_send, s_send, o_recv,
):
    rows, cols = q_hbm.shape
    heads = cols // HEAD_DIM
    group = rows // 2
    factor = math.log2(math.e) / math.sqrt(HEAD_DIM)
    me = lax.axis_index("blk")
    core = lax.rem(me, CORES)
    chip = lax.rem(me // CORES, heads)
    cell = me // (CORES * heads)

    def index(cc, ch, co):
        return (cc * heads + ch) * CORES + co

    partner = index(cell, chip, 1 - core)

    def facing(other, i):
        return lax.rem(i + (heads // 2) * (other < cell).astype(jnp.int32), heads)

    def head_columns(h):
        start = h * HEAD_DIM
        if not isinstance(h, int):
            start = pl.multiple_of(start, HEAD_DIM)
        return pl.ds(start, HEAD_DIM)

    def own_slot(ch, co):
        return ch * CORES + co

    q_loads = [pltpu.make_async_copy(q_hbm.at[:, head_columns(h)], stage_q.at[h], load_q) for h in range(heads)]
    kv_loads = []
    for h in range(heads):
        for part, source in enumerate((k_hbm, v_hbm)):
            place = stage_kv.at[h, :, pl.ds(part * HEAD_DIM, HEAD_DIM)]
            kv_loads.append(pltpu.make_async_copy(source.at[:, head_columns(h)], place, load_kv))
    own_kv = [
        pltpu.make_async_copy(
            source.at[:, head_columns(chip)],
            kv.at[own_slot(chip, core), :, pl.ds(part * HEAD_DIM, HEAD_DIM)],
            own_sem.at[0],
        )
        for part, source in enumerate((k_hbm, v_hbm))
    ]
    own_q = pltpu.make_async_copy(q_hbm.at[:, head_columns(chip)], qin.at[cell, chip], own_sem.at[1])
    small_loads = (
        pltpu.make_async_copy(table_hbm, table_ref, small_sem.at[0]),
        pltpu.make_async_copy(doc_hbm, doc_ref, small_sem.at[1]),
    )
    for one in small_loads:
        one.start()
    for one in kv_loads:
        one.start()
    for one in own_kv:
        one.start()
    for one in q_loads:
        one.start()
    own_q.start()

    barrier = pltpu.get_barrier_semaphore()
    peers = []
    for i in range(heads - 1, 0, -1):
        peers.append((cell, chip ^ i, i))
    for k in range(1, cells):
        other = lax.rem(cell + k, cells)
        for i in range(heads):
            peers.append((other, facing(other, i) ^ lax.rem(chip, 2), k * heads + i))
    mates = [one for one in peers if one[2] < heads]
    others = [one for one in peers if one[2] >= heads]
    for cc, ch, _ in mates:
        pl.semaphore_signal(barrier, inc=1, device_id={"blk": index(cc, ch, 0)})
    for cc, ch, _ in others:
        pl.semaphore_signal(barrier, inc=1, device_id={"blk": index(cc, ch, 1)})

    def greet_partner():
        pl.semaphore_signal(barrier, inc=1, device_id={"blk": partner})

    pl.when(core == 1)(greet_partner)

    def cell_here():
        def hear():
            pl.semaphore_wait(barrier, CORES * len(mates) + 1)
            pl.semaphore_signal(ready.at[0], inc=1, device_id={"blk": partner})

        pl.when(core == 0)(hear)
        pl.when(core == 1)(lambda: pl.semaphore_wait(ready.at[0], 1))

    def others_here():
        def hear():
            pl.semaphore_wait(barrier, CORES * len(others))
            pl.semaphore_signal(ready.at[1], inc=1, device_id={"blk": partner})

        pl.when(core == 1)(hear)
        pl.when(core == 0)(lambda: pl.semaphore_wait(ready.at[1], 1))

    for one in small_loads:
        one.wait()
    within = lax.broadcasted_iota(jnp.int32, (1, group), 1)
    for g in range(2):
        own_group = table_ref[0, g]
        meta[me, pl.ds(g, 1), :] = doc_ref[pl.ds(own_group, 1), :].astype(jnp.float32)
        meta[me, pl.ds(2 + g, 1), :] = (own_group * group + within).astype(jnp.float32)
    cell_here()

    def remote(src, dst, ssem, rsem, target):
        return pltpu.make_async_remote_copy(
            src_ref=src, dst_ref=dst, send_sem=ssem, recv_sem=rsem, device_id={"blk": target}
        )

    def q_copy(cc, ch):
        return remote(stage_q.at[ch], qin.at[cell, chip], q_send, q_recv.at[cell, chip], index(cc, ch, core))

    def kv_copy(ch):
        place = own_slot(chip, core)
        return remote(stage_kv.at[ch], kv.at[place], kv_send, kv_recv.at[place], index(cell, ch, core))

    def kv_forward(ch):
        place = own_slot(ch, core)
        return remote(kv.at[place], kv.at[place], fwd_send, kv_recv.at[place], partner)

    def near_meta(ch):
        place = own_slot(chip, core)
        return remote(meta.at[me], meta.at[me], m_send, kv_recv.at[place], index(cell, ch, core))

    def far_meta(cc, ch):
        return remote(meta.at[me], meta.at[me], m_send, q_recv.at[cell, chip], index(cc, ch, core))

    def meta_forward(ch):
        source = index(cell, ch, core)
        return remote(meta.at[source], meta.at[source], mf_send, kv_recv.at[own_slot(ch, core)], partner)

    def await_all(ref, sem):
        pltpu.make_async_copy(ref, ref, sem).wait()

    def await_rows(count, sem):
        await_all(measure.at[pl.ds(0, count)], sem)

    meta_rows = 2 * meta.shape[1]

    def kv_arrival(place):
        await_rows(2 * rows + meta_rows, kv_recv.at[place])

    near = [one for one in peers if one[2] < heads]
    far = [one for one in peers if one[2] >= heads]
    for cc, ch, n in near:
        near_meta(ch).start()
    meta_forward(chip).start()
    await_all(stage_kv, load_kv)
    for cc, ch, n in near:
        kv_copy(ch).start()
    await_all(kv.at[own_slot(chip, core)], own_sem.at[0])
    kv_forward(chip).start()
    await_all(stage_q, load_q)
    others_here()
    for cc, ch, n in far:
        far_meta(cc, ch).start()
    for cc, ch, n in far:
        q_copy(cc, ch).start()
    for cc, ch, n in near:
        q_copy(cc, ch).start()
    own_q.wait()
    for cc, ch, n in near:
        kv_arrival(own_slot(ch, core))
        kv_forward(ch).start()
        meta_forward(ch).start()
    for i in range(heads):
        kv_arrival(own_slot(lax.rem(chip + i, heads), 1 - core))

    sources = heads * CORES
    down = lax.broadcasted_iota(jnp.int32, (group, group), 0)
    right = lax.broadcasted_iota(jnp.int32, (group, group), 1)
    diagonal = down == right

    def to_rows(line):
        return jnp.sum(jnp.where(diagonal, line, 0.0), axis=1, keepdims=True)

    def to_lanes(column):
        return jnp.sum(jnp.where(diagonal, column, 0.0), axis=0, keepdims=True)

    def attend(cc, ch, home):
        order = [lax.rem(own_slot(ch, core) + i, sources) for i in range(sources)]
        q = qin[cc, ch]
        doc_line = [meta[home, pl.ds(slot, 1), :] for slot in range(2)]
        pos_line = [meta[home, pl.ds(2 + slot, 1), :] for slot in range(2)]
        doc = [jnp.broadcast_to(to_rows(one), (group, group)) for one in doc_line]
        pos = [jnp.broadcast_to(to_rows(one), (group, group)) for one in pos_line]
        parts = [[], []]
        for g in range(2):
            part = pl.ds(g * group, group)
            keys = jnp.concatenate([kv[s, part, pl.ds(0, HEAD_DIM)] for s in order], axis=0)
            scores = lax.dot_general(
                q if g == 0 else q[group:], keys, (((1,), (1,)), ((), ())), preferred_element_type=jnp.float32
            )
            for i, s in enumerate(order):
                key_doc = meta[cell * sources + s, pl.ds(g, 1), :]
                key_pos = meta[cell * sources + s, pl.ds(2 + g, 1), :]
                for slot in range(g, 2):
                    row = (slot - g) * group
                    block = scores[row:row + group, i * group:(i + 1) * group]
                    if i:
                        seen = jnp.where(key_pos < pos_line[slot], key_doc, -1.0) == doc[slot]
                    else:
                        seen = (key_doc == doc[slot]) & (key_pos <= pos[slot])
                    parts[slot].append(jnp.where(seen, block, MASKED))
        best = []
        weights = []
        sums = []
        for slot in range(2):
            top = functools.reduce(jnp.maximum, parts[slot])
            top = jnp.broadcast_to(jnp.max(top, axis=1, keepdims=True), (group, group))
            found = [jnp.exp2((one - top) * factor) for one in parts[slot]]
            total = jnp.sum(functools.reduce(jnp.add, found), axis=1, keepdims=True)
            best.append(to_lanes(top))
            sums.append(to_lanes(jnp.broadcast_to(total, (group, group))))
            weights.append([one.astype(jnp.bfloat16) for one in found])
        outs = []
        for g in range(2):
            part = pl.ds(g * group, group)
            vals = jnp.concatenate([kv[s, part, pl.ds(HEAD_DIM, HEAD_DIM)] for s in order], axis=0)
            lines = [jnp.concatenate(weights[slot][g * sources:(g + 1) * sources], axis=1) for slot in range(g, 2)]
            line = lines[0] if g else jnp.concatenate(lines, axis=0)
            outs.append(jnp.dot(line, vals, preferred_element_type=jnp.float32))
        return (outs[0][:group], outs[0][group:] + outs[1]), best, sums

    def o_copy(cc, ch, n):
        return remote(osend.at[n], obuf.at[cell, chip], o_send, o_recv.at[cell, chip], index(cc, ch, core))

    def s_copy(cc, ch, n):
        return remote(ssend.at[n], sbuf.at[cell, chip], s_send, o_recv.at[cell, chip], index(cc, ch, core))

    def place_of(t):
        cc = lax.rem(cell + 1 + t // heads, cells)
        return cc, facing(cc, lax.rem(t, heads))

    def serve(t, carry):
        cc, ch = place_of(t)
        home = index(cc, ch, core)
        other = home != me

        pl.when((cc == cell) & other)(lambda: await_rows(rows, q_recv.at[cc, ch]))
        pl.when(cc != cell)(lambda: await_rows(rows + meta_rows, q_recv.at[cc, ch]))
        outs, best, sums = attend(cc, ch, home)
        for slot in range(2):
            osend[t, pl.ds(slot * group, group), :] = outs[slot].astype(jnp.bfloat16)
            ssend[t, pl.ds(slot, 1), :] = best[slot]
            ssend[t, pl.ds(2 + slot, 1), :] = sums[slot]

        def give():
            o_copy(cc, ch, t).start()
            s_copy(cc, ch, t).start()

        pl.when(other)(give)
        return carry

    lax.fori_loop(0, cells * heads, serve, 0)

    own_turn = (cells - 1) * heads + chip
    obuf[cell, chip] = osend[own_turn]
    sbuf[cell, chip] = ssend[own_turn]

    for h in range(heads):
        for cc in range(cells):
            pl.when((cell != cc) | (chip != h))(lambda: await_rows(rows + meta_rows, o_recv.at[cc, h]))
        for slot in range(2):
            part = pl.ds(slot * group, group)
            tops = [sbuf[cc, h, pl.ds(slot, 1), :] for cc in range(cells)]
            sums = [sbuf[cc, h, pl.ds(2 + slot, 1), :] for cc in range(cells)]
            top = functools.reduce(jnp.maximum, tops)
            scale = [jnp.exp2((one - top) * factor) for one in tops]
            total = functools.reduce(jnp.add, [a * b for a, b in zip(scale, sums)])
            mixed = None
            for cc in range(cells):
                weight = to_rows(scale[cc] / total)
                term = obuf[cc, h, part, :].astype(jnp.float32) * weight
                mixed = term if mixed is None else mixed + term
            out_ref[part, pl.ds(h * HEAD_DIM, HEAD_DIM)] = mixed.astype(out_ref.dtype)

    sent = pl.ds(0, cells * heads - 1)
    await_all(osend.at[sent], q_send)
    await_all(meta.at[sent], m_send)
    await_all(kv.at[pl.ds(0, heads - 1)], kv_send)
    await_all(kv.at[pl.ds(0, heads)], fwd_send)
    await_all(meta.at[pl.ds(0, heads)], mf_send)
    await_all(osend.at[sent], o_send)
    await_all(ssend.at[sent], s_send)


def solution(mesh):
    members = mesh.shape["blk"]

    def shards(queries, keys, values, group_table, doc_ids):
        rows, cols = queries.shape
        group = rows // 2
        heads = cols // HEAD_DIM
        cells = members // (heads * CORES)
        doc_rows = doc_ids.reshape(-1, group)
        bf16, f32 = jnp.bfloat16, jnp.float32
        dma = pltpu.SemaphoreType.DMA
        return pl.pallas_call(
            functools.partial(attend_kernel, cells),
            out_shape=jax.ShapeDtypeStruct((rows, cols), bf16),
            in_specs=[pl.BlockSpec(memory_space=pl.ANY)] * 5,
            out_specs=pl.BlockSpec(memory_space=pltpu.VMEM),
            scratch_shapes=[
                pltpu.SMEM((1, 2), jnp.int32),
                pltpu.VMEM(doc_rows.shape, jnp.int32),
                pltpu.VMEM((heads, rows, HEAD_DIM), bf16),
                pltpu.VMEM((heads, rows, 2 * HEAD_DIM), bf16),
                pltpu.VMEM((cells, heads, rows, HEAD_DIM), bf16),
                pltpu.VMEM((heads * CORES, rows, 2 * HEAD_DIM), bf16),
                pltpu.VMEM((members, 4, group), f32),
                pltpu.VMEM((cells * heads, rows, HEAD_DIM), bf16),
                pltpu.VMEM((cells * heads, 4, group), f32),
                pltpu.VMEM((cells, heads, rows, HEAD_DIM), bf16),
                pltpu.VMEM((cells, heads, 4, group), f32),
                pltpu.VMEM((2 * (rows + 4), HEAD_DIM), bf16),
                pltpu.SemaphoreType.REGULAR((2,)),
                dma((2,)),
                dma,
                dma,
                dma((2,)),
                dma,
                dma((cells, heads)),
                dma,
                dma((heads * CORES,)),
                dma,
                dma,
                dma,
                dma,
                dma,
                dma((cells, heads)),
            ],
            compiler_params=pltpu.CompilerParams(
                collective_id=0, has_side_effects=True, vmem_limit_bytes=12 * 1024 * 1024
            ),
        )(*[pltpu.with_memory_space_constraint(one, pltpu.HBM) for one in (group_table, queries, keys, values, doc_rows)])

    in_specs = (P("blk", "head"), P("blk", "head"), P("blk", "head"), P("blk", None), P())
    return jax.shard_map(shards, mesh=mesh, in_specs=in_specs, out_specs=P("blk", "head"), check_vma=False)
```

```python
import functools
import math

import jax
import jax.numpy as jnp
from jax import lax
from jax.experimental import pallas as pl
from jax.experimental.pallas import tpu as pltpu
from jax.sharding import PartitionSpec as P

HEAD_DIM = 128
CORES = 2
MASKED = -1e30


def attend_kernel(
    cells, table_hbm, q_hbm, k_hbm, v_hbm, doc_hbm, out_ref,
    table_ref, doc_ref, stage_q, stage_kv, qin, kv, meta, osend, ssend, obuf, sbuf, measure,
    ready, small_sem, load_q, load_kv, own_sem, q_send, q_recv, kv_send, kv_recv, fwd_send, m_send, mf_send,
    o_send, s_send, o_recv,
):
    rows, cols = q_hbm.shape
    heads = cols // HEAD_DIM
    group = rows // 2
    factor = math.log2(math.e) / math.sqrt(HEAD_DIM)
    me = lax.axis_index("blk")
    core = lax.rem(me, CORES)
    chip = lax.rem(me // CORES, heads)
    cell = me // (CORES * heads)

    def index(cc, ch, co):
        return (cc * heads + ch) * CORES + co

    partner = index(cell, chip, 1 - core)

    half = heads // 2
    layer = chip // half
    inner = layer == (lax.rem(cell + 1, cells) > cell).astype(jnp.int32)

    def facing(other, i):
        return lax.rem(i + half * (other < cell).astype(jnp.int32), heads)

    def head_columns(h):
        start = h * HEAD_DIM
        if not isinstance(h, int):
            start = pl.multiple_of(start, HEAD_DIM)
        return pl.ds(start, HEAD_DIM)

    def own_slot(ch, co):
        return ch * CORES + co

    q_loads = [pltpu.make_async_copy(q_hbm.at[:, head_columns(h)], stage_q.at[h], load_q) for h in range(heads)]
    kv_loads = []
    for h in range(heads):
        for part, source in enumerate((k_hbm, v_hbm)):
            place = stage_kv.at[h, :, pl.ds(part * HEAD_DIM, HEAD_DIM)]
            kv_loads.append(pltpu.make_async_copy(source.at[:, head_columns(h)], place, load_kv))
    own_kv = [
        pltpu.make_async_copy(
            source.at[:, head_columns(chip)],
            kv.at[own_slot(chip, core), :, pl.ds(part * HEAD_DIM, HEAD_DIM)],
            own_sem.at[0],
        )
        for part, source in enumerate((k_hbm, v_hbm))
    ]
    own_q = pltpu.make_async_copy(q_hbm.at[:, head_columns(chip)], qin.at[cell, chip], own_sem.at[1])
    small_loads = (
        pltpu.make_async_copy(table_hbm, table_ref, small_sem.at[0]),
        pltpu.make_async_copy(doc_hbm, doc_ref, small_sem.at[1]),
    )
    for one in small_loads:
        one.start()
    for one in kv_loads:
        one.start()
    for one in own_kv:
        one.start()
    for one in q_loads:
        one.start()
    own_q.start()

    barrier = pltpu.get_barrier_semaphore()
    peers = []
    for i in range(heads - 1, 0, -1):
        peers.append((cell, chip ^ i, i))
    for k in range(1, cells):
        other = lax.rem(cell + k, cells)
        for i in range(heads):
            peers.append((other, facing(other, i) ^ lax.rem(chip, 2), k * heads + i))
    mates = [one for one in peers if one[2] < heads]
    others = [one for one in peers if one[2] >= heads]
    for cc, ch, _ in mates:
        pl.semaphore_signal(barrier, inc=1, device_id={"blk": index(cc, ch, 0)})
    for cc, ch, _ in others:
        pl.semaphore_signal(barrier, inc=1, device_id={"blk": index(cc, ch, 1)})

    def greet_partner():
        pl.semaphore_signal(barrier, inc=1, device_id={"blk": partner})

    pl.when(core == 1)(greet_partner)

    def cell_here():
        def hear():
            pl.semaphore_wait(barrier, CORES * len(mates) + 1)
            pl.semaphore_signal(ready.at[0], inc=1, device_id={"blk": partner})

        pl.when(core == 0)(hear)
        pl.when(core == 1)(lambda: pl.semaphore_wait(ready.at[0], 1))

    def others_here():
        def hear():
            pl.semaphore_wait(barrier, CORES * len(others))
            pl.semaphore_signal(ready.at[1], inc=1, device_id={"blk": partner})

        pl.when(core == 1)(hear)
        pl.when(core == 0)(lambda: pl.semaphore_wait(ready.at[1], 1))

    for one in small_loads:
        one.wait()
    within = lax.broadcasted_iota(jnp.int32, (1, group), 1)
    for g in range(2):
        own_group = table_ref[0, g]
        meta[me, pl.ds(g, 1), :] = doc_ref[pl.ds(own_group, 1), :].astype(jnp.float32)
        meta[me, pl.ds(2 + g, 1), :] = (own_group * group + within).astype(jnp.float32)
    cell_here()

    def remote(src, dst, ssem, rsem, target):
        return pltpu.make_async_remote_copy(
            src_ref=src, dst_ref=dst, send_sem=ssem, recv_sem=rsem, device_id={"blk": target}
        )

    def q_copy(cc, ch):
        return remote(stage_q.at[ch], qin.at[cell, chip], q_send, q_recv.at[cell, chip], index(cc, ch, core))

    def kv_copy(ch):
        place = own_slot(chip, core)
        return remote(stage_kv.at[ch], kv.at[place], kv_send, kv_recv.at[place], index(cell, ch, core))

    def kv_forward(ch):
        place = own_slot(ch, core)
        return remote(kv.at[place], kv.at[place], fwd_send, kv_recv.at[place], partner)

    def near_meta(ch):
        place = own_slot(chip, core)
        return remote(meta.at[me], meta.at[me], m_send, kv_recv.at[place], index(cell, ch, core))

    def far_meta(cc, ch):
        return remote(meta.at[me], meta.at[me], m_send, q_recv.at[cell, chip], index(cc, ch, core))

    def meta_forward(ch):
        source = index(cell, ch, core)
        return remote(meta.at[source], meta.at[source], mf_send, kv_recv.at[own_slot(ch, core)], partner)

    def await_all(ref, sem):
        pltpu.make_async_copy(ref, ref, sem).wait()

    def await_rows(count, sem):
        await_all(measure.at[pl.ds(0, count)], sem)

    meta_rows = 2 * meta.shape[1]

    def kv_arrival(place):
        await_rows(2 * rows + meta_rows, kv_recv.at[place])

    near = [one for one in peers if one[2] < heads]
    far = [one for one in peers if one[2] >= heads]
    for cc, ch, n in near:
        near_meta(ch).start()
    meta_forward(chip).start()
    await_all(stage_kv, load_kv)
    for cc, ch, n in near:
        kv_copy(ch).start()
    await_all(kv.at[own_slot(chip, core)], own_sem.at[0])
    kv_forward(chip).start()
    await_all(stage_q, load_q)
    others_here()
    for cc, ch, n in far:
        far_meta(cc, ch).start()
    for cc, ch, n in far:
        q_copy(cc, ch).start()
    for cc, ch, n in near:
        q_copy(cc, ch).start()
    own_q.wait()
    for cc, ch, n in near:
        kv_arrival(own_slot(ch, core))
        kv_forward(ch).start()
        meta_forward(ch).start()
    for i in range(heads):
        kv_arrival(own_slot(lax.rem(chip + i, heads), 1 - core))

    sources = heads * CORES
    down = lax.broadcasted_iota(jnp.int32, (group, group), 0)
    right = lax.broadcasted_iota(jnp.int32, (group, group), 1)
    diagonal = down == right

    def to_rows(line):
        return jnp.sum(jnp.where(diagonal, line, 0.0), axis=1, keepdims=True)

    def to_lanes(column):
        return jnp.sum(jnp.where(diagonal, column, 0.0), axis=0, keepdims=True)

    def attend(cc, ch, home):
        order = [lax.rem(own_slot(ch, core) + i, sources) for i in range(sources)]
        q = qin[cc, ch]
        doc_line = [meta[home, pl.ds(slot, 1), :] for slot in range(2)]
        pos_line = [meta[home, pl.ds(2 + slot, 1), :] for slot in range(2)]
        doc = [jnp.broadcast_to(to_rows(one), (group, group)) for one in doc_line]
        pos = [jnp.broadcast_to(to_rows(one), (group, group)) for one in pos_line]
        parts = [[], []]
        for g in range(2):
            part = pl.ds(g * group, group)
            keys = jnp.concatenate([kv[s, part, pl.ds(0, HEAD_DIM)] for s in order], axis=0)
            scores = lax.dot_general(
                q if g == 0 else q[group:], keys, (((1,), (1,)), ((), ())), preferred_element_type=jnp.float32
            )
            for i, s in enumerate(order):
                key_doc = meta[cell * sources + s, pl.ds(g, 1), :]
                key_pos = meta[cell * sources + s, pl.ds(2 + g, 1), :]
                for slot in range(g, 2):
                    row = (slot - g) * group
                    block = scores[row:row + group, i * group:(i + 1) * group]
                    if i:
                        seen = jnp.where(key_pos < pos_line[slot], key_doc, -1.0) == doc[slot]
                    else:
                        seen = (key_doc == doc[slot]) & (key_pos <= pos[slot])
                    parts[slot].append(jnp.where(seen, block, MASKED))
        best = []
        weights = []
        sums = []
        for slot in range(2):
            top = functools.reduce(jnp.maximum, parts[slot])
            top = jnp.broadcast_to(jnp.max(top, axis=1, keepdims=True), (group, group))
            found = [jnp.exp2((one - top) * factor) for one in parts[slot]]
            total = jnp.sum(functools.reduce(jnp.add, found), axis=1, keepdims=True)
            best.append(to_lanes(top))
            sums.append(to_lanes(jnp.broadcast_to(total, (group, group))))
            weights.append([one.astype(jnp.bfloat16) for one in found])
        outs = []
        for g in range(2):
            part = pl.ds(g * group, group)
            vals = jnp.concatenate([kv[s, part, pl.ds(HEAD_DIM, HEAD_DIM)] for s in order], axis=0)
            lines = [jnp.concatenate(weights[slot][g * sources:(g + 1) * sources], axis=1) for slot in range(g, 2)]
            line = lines[0] if g else jnp.concatenate(lines, axis=0)
            outs.append(jnp.dot(line, vals, preferred_element_type=jnp.float32))
        return (outs[0][:group], outs[0][group:] + outs[1]), best, sums

    def o_copy(cc, ch, n):
        return remote(osend.at[n], obuf.at[cell, chip], o_send, o_recv.at[cell, chip], index(cc, ch, core))

    def s_copy(cc, ch, n):
        return remote(ssend.at[n], sbuf.at[cell, chip], s_send, o_recv.at[cell, chip], index(cc, ch, core))

    cross_block = jnp.where(inner, 2, 3)
    own_block = jnp.where(inner, 3, 2)

    def place_of(t):
        block, step = t // half, lax.rem(t, half)
        is_cross, is_own = block == cross_block, block == own_block
        far_block = block - (cross_block < block).astype(jnp.int32) - (own_block < block).astype(jnp.int32)
        other = lax.rem(cell + 1 + far_block // 2, cells)
        far_layer = lax.rem(far_block + (inner).astype(jnp.int32), 2)
        far_chip = facing(other, far_layer * half + step)
        own_chip = layer * half + lax.rem(lax.rem(chip, half) + 1 + step, half)
        near_chip = jnp.where(is_own, own_chip, (1 - layer) * half + step)
        near_cell = is_cross | is_own
        return jnp.where(near_cell, cell, other), jnp.where(near_cell, near_chip, far_chip)

    def serve(t, carry):
        cc, ch = place_of(t)
        home = index(cc, ch, core)
        other = home != me

        pl.when((cc == cell) & other)(lambda: await_rows(rows, q_recv.at[cc, ch]))
        pl.when(cc != cell)(lambda: await_rows(rows + meta_rows, q_recv.at[cc, ch]))
        outs, best, sums = attend(cc, ch, home)
        for slot in range(2):
            osend[t, pl.ds(slot * group, group), :] = outs[slot].astype(jnp.bfloat16)
            ssend[t, pl.ds(slot, 1), :] = best[slot]
            ssend[t, pl.ds(2 + slot, 1), :] = sums[slot]

        def give():
            o_copy(cc, ch, t).start()
            s_copy(cc, ch, t).start()

        pl.when(other)(give)
        return carry

    lax.fori_loop(0, cells * heads, serve, 0)

    own_turn = own_block * half + half - 1
    obuf[cell, chip] = osend[own_turn]
    sbuf[cell, chip] = ssend[own_turn]

    for h in range(heads):
        for cc in range(cells):
            pl.when((cell != cc) | (chip != h))(lambda: await_rows(rows + meta_rows, o_recv.at[cc, h]))
        for slot in range(2):
            part = pl.ds(slot * group, group)
            tops = [sbuf[cc, h, pl.ds(slot, 1), :] for cc in range(cells)]
            sums = [sbuf[cc, h, pl.ds(2 + slot, 1), :] for cc in range(cells)]
            top = functools.reduce(jnp.maximum, tops)
            scale = [jnp.exp2((one - top) * factor) for one in tops]
            total = functools.reduce(jnp.add, [a * b for a, b in zip(scale, sums)])
            mixed = None
            for cc in range(cells):
                weight = to_rows(scale[cc] / total)
                term = obuf[cc, h, part, :].astype(jnp.float32) * weight
                mixed = term if mixed is None else mixed + term
            out_ref[part, pl.ds(h * HEAD_DIM, HEAD_DIM)] = mixed.astype(out_ref.dtype)

    sent = pl.ds(0, cells * heads - 1)
    await_all(osend.at[sent], q_send)
    await_all(meta.at[sent], m_send)
    await_all(kv.at[pl.ds(0, heads - 1)], kv_send)
    await_all(kv.at[pl.ds(0, heads)], fwd_send)
    await_all(meta.at[pl.ds(0, heads)], mf_send)
    await_all(osend.at[sent], o_send)
    await_all(ssend.at[sent], s_send)


def solution(mesh):
    members = mesh.shape["blk"]

    def shards(queries, keys, values, group_table, doc_ids):
        rows, cols = queries.shape
        group = rows // 2
        heads = cols // HEAD_DIM
        cells = members // (heads * CORES)
        doc_rows = doc_ids.reshape(-1, group)
        bf16, f32 = jnp.bfloat16, jnp.float32
        dma = pltpu.SemaphoreType.DMA
        return pl.pallas_call(
            functools.partial(attend_kernel, cells),
            out_shape=jax.ShapeDtypeStruct((rows, cols), bf16),
            in_specs=[pl.BlockSpec(memory_space=pl.ANY)] * 5,
            out_specs=pl.BlockSpec(memory_space=pltpu.VMEM),
            scratch_shapes=[
                pltpu.SMEM((1, 2), jnp.int32),
                pltpu.VMEM(doc_rows.shape, jnp.int32),
                pltpu.VMEM((heads, rows, HEAD_DIM), bf16),
                pltpu.VMEM((heads, rows, 2 * HEAD_DIM), bf16),
                pltpu.VMEM((cells, heads, rows, HEAD_DIM), bf16),
                pltpu.VMEM((heads * CORES, rows, 2 * HEAD_DIM), bf16),
                pltpu.VMEM((members, 4, group), f32),
                pltpu.VMEM((cells * heads, rows, HEAD_DIM), bf16),
                pltpu.VMEM((cells * heads, 4, group), f32),
                pltpu.VMEM((cells, heads, rows, HEAD_DIM), bf16),
                pltpu.VMEM((cells, heads, 4, group), f32),
                pltpu.VMEM((2 * (rows + 4), HEAD_DIM), bf16),
                pltpu.SemaphoreType.REGULAR((2,)),
                dma((2,)),
                dma,
                dma,
                dma((2,)),
                dma,
                dma((cells, heads)),
                dma,
                dma((heads * CORES,)),
                dma,
                dma,
                dma,
                dma,
                dma,
                dma((cells, heads)),
            ],
            compiler_params=pltpu.CompilerParams(
                collective_id=0, has_side_effects=True, vmem_limit_bytes=12 * 1024 * 1024
            ),
        )(*[pltpu.with_memory_space_constraint(one, pltpu.HBM) for one in (group_table, queries, keys, values, doc_rows)])

    in_specs = (P("blk", "head"), P("blk", "head"), P("blk", "head"), P("blk", None), P())
    return jax.shard_map(shards, mesh=mesh, in_specs=in_specs, out_specs=P("blk", "head"), check_vma=False)
```

```python
import functools
import math

import jax
import jax.numpy as jnp
from jax import lax
from jax.experimental import pallas as pl
from jax.experimental.pallas import tpu as pltpu
from jax.sharding import PartitionSpec as P

HEAD_DIM = 128
CORES = 2
MASKED = -1e30


def attend_kernel(
    cells, table_hbm, q_hbm, k_hbm, v_hbm, doc_hbm, out_ref,
    table_ref, doc_ref, stage_q, stage_kv, qin, kv, meta, osend, ssend, obuf, sbuf, measure,
    ready, small_sem, load_q, load_kv, own_sem, q_send, q_recv, kv_send, kv_recv, fwd_send, m_send, mf_send,
    o_send, s_send, o_recv,
):
    rows, cols = q_hbm.shape
    heads = cols // HEAD_DIM
    group = rows // 2
    factor = math.log2(math.e) / math.sqrt(HEAD_DIM)
    me = lax.axis_index("blk")
    core = lax.rem(me, CORES)
    chip = lax.rem(me // CORES, heads)
    cell = me // (CORES * heads)

    def index(cc, ch, co):
        return (cc * heads + ch) * CORES + co

    partner = index(cell, chip, 1 - core)

    half = heads // 2
    layer = chip // half
    inner = layer == (lax.rem(cell + 1, cells) > cell).astype(jnp.int32)

    def facing(other, i):
        return lax.rem(i + half * (other < cell).astype(jnp.int32), heads)

    def head_columns(h):
        start = h * HEAD_DIM
        if not isinstance(h, int):
            start = pl.multiple_of(start, HEAD_DIM)
        return pl.ds(start, HEAD_DIM)

    def own_slot(ch, co):
        return ch * CORES + co

    q_loads = [pltpu.make_async_copy(q_hbm.at[:, head_columns(h)], stage_q.at[h], load_q) for h in range(heads)]
    kv_loads = []
    for h in range(heads):
        for part, source in enumerate((k_hbm, v_hbm)):
            place = stage_kv.at[h, :, pl.ds(part * HEAD_DIM, HEAD_DIM)]
            kv_loads.append(pltpu.make_async_copy(source.at[:, head_columns(h)], place, load_kv))
    own_kv = [
        pltpu.make_async_copy(
            source.at[:, head_columns(chip)],
            kv.at[own_slot(chip, core), :, pl.ds(part * HEAD_DIM, HEAD_DIM)],
            own_sem.at[0],
        )
        for part, source in enumerate((k_hbm, v_hbm))
    ]
    own_q = pltpu.make_async_copy(q_hbm.at[:, head_columns(chip)], qin.at[cell, chip], own_sem.at[1])
    small_loads = (
        pltpu.make_async_copy(table_hbm, table_ref, small_sem.at[0]),
        pltpu.make_async_copy(doc_hbm, doc_ref, small_sem.at[1]),
    )
    for one in small_loads:
        one.start()
    for one in kv_loads:
        one.start()
    for one in own_kv:
        one.start()
    for one in q_loads:
        one.start()
    own_q.start()

    barrier = pltpu.get_barrier_semaphore()
    peers = []
    for i in range(heads - 1, 0, -1):
        peers.append((cell, chip ^ i, i))
    for k in range(1, cells):
        other = lax.rem(cell + k, cells)
        for i in range(heads):
            peers.append((other, facing(other, i) ^ lax.rem(chip, 2), k * heads + i))
    mates = [one for one in peers if one[2] < heads]
    others = [one for one in peers if one[2] >= heads]
    for cc, ch, _ in mates:
        pl.semaphore_signal(barrier, inc=1, device_id={"blk": index(cc, ch, 0)})
    for cc, ch, _ in others:
        pl.semaphore_signal(barrier, inc=1, device_id={"blk": index(cc, ch, 1)})

    def greet_partner():
        pl.semaphore_signal(barrier, inc=1, device_id={"blk": partner})

    pl.when(core == 1)(greet_partner)

    def cell_here():
        def hear():
            pl.semaphore_wait(barrier, CORES * len(mates) + 1)
            pl.semaphore_signal(ready.at[0], inc=1, device_id={"blk": partner})

        pl.when(core == 0)(hear)
        pl.when(core == 1)(lambda: pl.semaphore_wait(ready.at[0], 1))

    def others_here():
        def hear():
            pl.semaphore_wait(barrier, CORES * len(others))
            pl.semaphore_signal(ready.at[1], inc=1, device_id={"blk": partner})

        pl.when(core == 1)(hear)
        pl.when(core == 0)(lambda: pl.semaphore_wait(ready.at[1], 1))

    for one in small_loads:
        one.wait()
    within = lax.broadcasted_iota(jnp.int32, (1, group), 1)
    for g in range(2):
        own_group = table_ref[0, g]
        meta[me, pl.ds(g, 1), :] = doc_ref[pl.ds(own_group, 1), :].astype(jnp.float32)
        meta[me, pl.ds(2 + g, 1), :] = (own_group * group + within).astype(jnp.float32)
    cell_here()

    def remote(src, dst, ssem, rsem, target):
        return pltpu.make_async_remote_copy(
            src_ref=src, dst_ref=dst, send_sem=ssem, recv_sem=rsem, device_id={"blk": target}
        )

    def q_copy(cc, ch):
        return remote(stage_q.at[ch], qin.at[cell, chip], q_send, q_recv.at[cell, chip], index(cc, ch, core))

    def kv_copy(ch):
        place = own_slot(chip, core)
        return remote(stage_kv.at[ch], kv.at[place], kv_send, kv_recv.at[place], index(cell, ch, core))

    def kv_forward(ch):
        place = own_slot(ch, core)
        return remote(kv.at[place], kv.at[place], fwd_send, kv_recv.at[place], partner)

    def near_meta(ch):
        place = own_slot(chip, core)
        return remote(meta.at[me], meta.at[me], m_send, kv_recv.at[place], index(cell, ch, core))

    def far_meta(cc, ch):
        return remote(meta.at[me], meta.at[me], m_send, q_recv.at[cell, chip], index(cc, ch, core))

    def meta_forward(ch):
        source = index(cell, ch, core)
        return remote(meta.at[source], meta.at[source], mf_send, kv_recv.at[own_slot(ch, core)], partner)

    def await_all(ref, sem):
        pltpu.make_async_copy(ref, ref, sem).wait()

    def await_rows(count, sem):
        await_all(measure.at[pl.ds(0, count)], sem)

    meta_rows = 2 * meta.shape[1]

    def kv_arrival(place):
        await_rows(2 * rows + meta_rows, kv_recv.at[place])

    near = [one for one in peers if one[2] < heads]
    far = [one for one in peers if one[2] >= heads]
    for cc, ch, n in near:
        near_meta(ch).start()
    meta_forward(chip).start()
    await_all(stage_kv, load_kv)
    for cc, ch, n in near:
        kv_copy(ch).start()
    await_all(kv.at[own_slot(chip, core)], own_sem.at[0])
    kv_forward(chip).start()
    await_all(stage_q, load_q)
    others_here()
    for cc, ch, n in far:
        far_meta(cc, ch).start()
    for cc, ch, n in far:
        q_copy(cc, ch).start()
    for cc, ch, n in near:
        q_copy(cc, ch).start()
    own_q.wait()
    for cc, ch, n in near:
        kv_arrival(own_slot(ch, core))
        kv_forward(ch).start()
        meta_forward(ch).start()
    for i in range(heads):
        kv_arrival(own_slot(lax.rem(chip + i, heads), 1 - core))

    sources = heads * CORES
    down = lax.broadcasted_iota(jnp.int32, (group, group), 0)
    right = lax.broadcasted_iota(jnp.int32, (group, group), 1)
    diagonal = down == right

    def to_rows(line):
        return jnp.sum(jnp.where(diagonal, line, 0.0), axis=1, keepdims=True)

    def to_lanes(column):
        return jnp.sum(jnp.where(diagonal, column, 0.0), axis=0, keepdims=True)

    def attend(cc, ch, home):
        order = [lax.rem(own_slot(ch, core) + i, sources) for i in range(sources)]
        q = qin[cc, ch]
        doc_line = [meta[home, pl.ds(slot, 1), :] for slot in range(2)]
        pos_line = [meta[home, pl.ds(2 + slot, 1), :] for slot in range(2)]
        doc = [jnp.broadcast_to(to_rows(one), (group, group)) for one in doc_line]
        pos = [jnp.broadcast_to(to_rows(one), (group, group)) for one in pos_line]
        parts = [[], []]
        for g in range(2):
            part = pl.ds(g * group, group)
            keys = jnp.concatenate([kv[s, part, pl.ds(0, HEAD_DIM)] for s in order], axis=0)
            scores = lax.dot_general(
                q if g == 0 else q[group:], keys, (((1,), (1,)), ((), ())), preferred_element_type=jnp.float32
            )
            for i, s in enumerate(order):
                key_doc = meta[cell * sources + s, pl.ds(g, 1), :]
                key_pos = meta[cell * sources + s, pl.ds(2 + g, 1), :]
                for slot in range(g, 2):
                    row = (slot - g) * group
                    block = scores[row:row + group, i * group:(i + 1) * group]
                    if i:
                        seen = jnp.where(key_pos < pos_line[slot], key_doc, -1.0) == doc[slot]
                    else:
                        seen = (key_doc == doc[slot]) & (key_pos <= pos[slot])
                    parts[slot].append(jnp.where(seen, block, MASKED))
        best = []
        weights = []
        sums = []
        for slot in range(2):
            top = functools.reduce(jnp.maximum, parts[slot])
            top = jnp.broadcast_to(jnp.max(top, axis=1, keepdims=True), (group, group))
            found = [jnp.exp2((one - top) * factor) for one in parts[slot]]
            total = jnp.sum(functools.reduce(jnp.add, found), axis=1, keepdims=True)
            best.append(to_lanes(top))
            sums.append(to_lanes(jnp.broadcast_to(total, (group, group))))
            weights.append([one.astype(jnp.bfloat16) for one in found])
        outs = []
        for g in range(2):
            part = pl.ds(g * group, group)
            vals = jnp.concatenate([kv[s, part, pl.ds(HEAD_DIM, HEAD_DIM)] for s in order], axis=0)
            lines = [jnp.concatenate(weights[slot][g * sources:(g + 1) * sources], axis=1) for slot in range(g, 2)]
            line = lines[0] if g else jnp.concatenate(lines, axis=0)
            outs.append(jnp.dot(line, vals, preferred_element_type=jnp.float32))
        return (outs[0][:group], outs[0][group:] + outs[1]), best, sums

    def o_copy(cc, ch, n):
        return remote(osend.at[n], obuf.at[cell, chip], o_send, o_recv.at[cell, chip], index(cc, ch, core))

    def s_copy(cc, ch, n):
        return remote(ssend.at[n], sbuf.at[cell, chip], s_send, o_recv.at[cell, chip], index(cc, ch, core))

    cross_block = jnp.where(inner, 2, 3)
    own_block = jnp.where(inner, 3, 2)

    def place_of(t):
        block, step = t // half, lax.rem(t, half)
        is_cross, is_own = block == cross_block, block == own_block
        far_block = block - (cross_block < block).astype(jnp.int32) - (own_block < block).astype(jnp.int32)
        other = lax.rem(cell + 1 + far_block // 2, cells)
        far_layer = lax.rem(far_block + (inner).astype(jnp.int32), 2)
        far_chip = facing(other, far_layer * half + step)
        own_chip = layer * half + lax.rem(lax.rem(chip, half) + 1 + step, half)
        near_chip = jnp.where(is_own, own_chip, (1 - layer) * half + step)
        near_cell = is_cross | is_own
        return jnp.where(near_cell, cell, other), jnp.where(near_cell, near_chip, far_chip)

    def serve(t, carry):
        cc, ch = place_of(t)
        home = index(cc, ch, core)
        other = home != me

        pl.when((cc == cell) & other)(lambda: await_rows(rows, q_recv.at[cc, ch]))
        pl.when(cc != cell)(lambda: await_rows(rows + meta_rows, q_recv.at[cc, ch]))
        outs, best, sums = attend(cc, ch, home)
        for slot in range(2):
            osend[t, pl.ds(slot * group, group), :] = outs[slot].astype(jnp.bfloat16)
            ssend[t, pl.ds(slot, 1), :] = best[slot]
            ssend[t, pl.ds(2 + slot, 1), :] = sums[slot]

        def give():
            o_copy(cc, ch, t).start()
            s_copy(cc, ch, t).start()

        pl.when(other)(give)
        return carry

    lax.fori_loop(0, cells * heads, serve, 0)

    own_turn = own_block * half + half - 1
    obuf[cell, chip] = osend[own_turn]
    sbuf[cell, chip] = ssend[own_turn]

    for i in range(heads):
        h = lax.rem(layer * half + i, heads)
        for cc in range(cells):
            pl.when((cell != cc) | (chip != h))(lambda: await_rows(rows + meta_rows, o_recv.at[cc, h]))
        for slot in range(2):
            part = pl.ds(slot * group, group)
            tops = [sbuf[cc, h, pl.ds(slot, 1), :] for cc in range(cells)]
            sums = [sbuf[cc, h, pl.ds(2 + slot, 1), :] for cc in range(cells)]
            top = functools.reduce(jnp.maximum, tops)
            scale = [jnp.exp2((one - top) * factor) for one in tops]
            total = functools.reduce(jnp.add, [a * b for a, b in zip(scale, sums)])
            mixed = None
            for cc in range(cells):
                weight = to_rows(scale[cc] / total)
                term = obuf[cc, h, part, :].astype(jnp.float32) * weight
                mixed = term if mixed is None else mixed + term
            out_ref[part, head_columns(h)] = mixed.astype(out_ref.dtype)

    sent = pl.ds(0, cells * heads - 1)
    await_all(osend.at[sent], q_send)
    await_all(meta.at[sent], m_send)
    await_all(kv.at[pl.ds(0, heads - 1)], kv_send)
    await_all(kv.at[pl.ds(0, heads)], fwd_send)
    await_all(meta.at[pl.ds(0, heads)], mf_send)
    await_all(osend.at[sent], o_send)
    await_all(ssend.at[sent], s_send)


def solution(mesh):
    members = mesh.shape["blk"]

    def shards(queries, keys, values, group_table, doc_ids):
        rows, cols = queries.shape
        group = rows // 2
        heads = cols // HEAD_DIM
        cells = members // (heads * CORES)
        doc_rows = doc_ids.reshape(-1, group)
        bf16, f32 = jnp.bfloat16, jnp.float32
        dma = pltpu.SemaphoreType.DMA
        return pl.pallas_call(
            functools.partial(attend_kernel, cells),
            out_shape=jax.ShapeDtypeStruct((rows, cols), bf16),
            in_specs=[pl.BlockSpec(memory_space=pl.ANY)] * 5,
            out_specs=pl.BlockSpec(memory_space=pltpu.VMEM),
            scratch_shapes=[
                pltpu.SMEM((1, 2), jnp.int32),
                pltpu.VMEM(doc_rows.shape, jnp.int32),
                pltpu.VMEM((heads, rows, HEAD_DIM), bf16),
                pltpu.VMEM((heads, rows, 2 * HEAD_DIM), bf16),
                pltpu.VMEM((cells, heads, rows, HEAD_DIM), bf16),
                pltpu.VMEM((heads * CORES, rows, 2 * HEAD_DIM), bf16),
                pltpu.VMEM((members, 4, group), f32),
                pltpu.VMEM((cells * heads, rows, HEAD_DIM), bf16),
                pltpu.VMEM((cells * heads, 4, group), f32),
                pltpu.VMEM((cells, heads, rows, HEAD_DIM), bf16),
                pltpu.VMEM((cells, heads, 4, group), f32),
                pltpu.VMEM((2 * (rows + 4), HEAD_DIM), bf16),
                pltpu.SemaphoreType.REGULAR((2,)),
                dma((2,)),
                dma,
                dma,
                dma((2,)),
                dma,
                dma((cells, heads)),
                dma,
                dma((heads * CORES,)),
                dma,
                dma,
                dma,
                dma,
                dma,
                dma((cells, heads)),
            ],
            compiler_params=pltpu.CompilerParams(
                collective_id=0, has_side_effects=True, vmem_limit_bytes=12 * 1024 * 1024
            ),
        )(*[pltpu.with_memory_space_constraint(one, pltpu.HBM) for one in (group_table, queries, keys, values, doc_rows)])

    in_specs = (P("blk", "head"), P("blk", "head"), P("blk", "head"), P("blk", None), P())
    return jax.shard_map(shards, mesh=mesh, in_specs=in_specs, out_specs=P("blk", "head"), check_vma=False)
```

```python
import functools
import math

import jax
import jax.numpy as jnp
from jax import lax
from jax.experimental import pallas as pl
from jax.experimental.pallas import tpu as pltpu
from jax.sharding import PartitionSpec as P

HEAD_DIM = 128
CORES = 2
MASKED = -1e30


def attend_kernel(
    cells, table_hbm, q_hbm, k_hbm, v_hbm, doc_hbm, out_ref,
    table_ref, doc_ref, stage_q, stage_kv, qin, kv, meta, osend, ssend, obuf, sbuf, measure,
    ready, small_sem, load_q, load_kv, own_sem, q_send, q_recv, kv_send, kv_recv, fwd_send, m_send, mf_send,
    o_send, s_send, o_recv,
):
    rows, cols = q_hbm.shape
    heads = cols // HEAD_DIM
    group = rows // 2
    factor = math.log2(math.e) / math.sqrt(HEAD_DIM)
    me = lax.axis_index("blk")
    core = lax.rem(me, CORES)
    chip = lax.rem(me // CORES, heads)
    cell = me // (CORES * heads)

    def index(cc, ch, co):
        return (cc * heads + ch) * CORES + co

    partner = index(cell, chip, 1 - core)

    half = heads // 2
    layer = chip // half
    inner = layer == (lax.rem(cell + 1, cells) > cell).astype(jnp.int32)

    def facing(other, i):
        return lax.rem(i + half * (other < cell).astype(jnp.int32), heads)

    def head_columns(h):
        start = h * HEAD_DIM
        if not isinstance(h, int):
            start = pl.multiple_of(start, HEAD_DIM)
        return pl.ds(start, HEAD_DIM)

    def own_slot(ch, co):
        return ch * CORES + co

    q_loads = [pltpu.make_async_copy(q_hbm.at[:, head_columns(h)], stage_q.at[h], load_q) for h in range(heads)]
    kv_loads = []
    for h in range(heads):
        for part, source in enumerate((k_hbm, v_hbm)):
            place = stage_kv.at[h, :, pl.ds(part * HEAD_DIM, HEAD_DIM)]
            kv_loads.append(pltpu.make_async_copy(source.at[:, head_columns(h)], place, load_kv))
    own_kv = [
        pltpu.make_async_copy(
            source.at[:, head_columns(chip)],
            kv.at[own_slot(chip, core), :, pl.ds(part * HEAD_DIM, HEAD_DIM)],
            own_sem.at[0],
        )
        for part, source in enumerate((k_hbm, v_hbm))
    ]
    own_q = pltpu.make_async_copy(q_hbm.at[:, head_columns(chip)], qin.at[cell, chip], own_sem.at[1])
    small_loads = (
        pltpu.make_async_copy(table_hbm, table_ref, small_sem.at[0]),
        pltpu.make_async_copy(doc_hbm, doc_ref, small_sem.at[1]),
    )
    for one in small_loads:
        one.start()
    for one in kv_loads:
        one.start()
    for one in own_kv:
        one.start()
    for one in q_loads:
        one.start()
    own_q.start()

    barrier = pltpu.get_barrier_semaphore()
    peers = []
    for i in range(heads - 1, 0, -1):
        peers.append((cell, chip ^ i, i))
    for k in range(1, cells):
        other = lax.rem(cell + k, cells)
        for i in range(heads):
            peers.append((other, facing(other, i) ^ lax.rem(chip, 2), k * heads + i))
    mates = [one for one in peers if one[2] < heads]
    others = [one for one in peers if one[2] >= heads]
    for cc, ch, _ in mates:
        pl.semaphore_signal(barrier, inc=1, device_id={"blk": index(cc, ch, 0)})
    for cc, ch, _ in others:
        pl.semaphore_signal(barrier, inc=1, device_id={"blk": index(cc, ch, 1)})

    def greet_partner():
        pl.semaphore_signal(barrier, inc=1, device_id={"blk": partner})

    pl.when(core == 1)(greet_partner)

    def cell_here():
        def hear():
            pl.semaphore_wait(barrier, CORES * len(mates) + 1)
            pl.semaphore_signal(ready.at[0], inc=1, device_id={"blk": partner})

        pl.when(core == 0)(hear)
        pl.when(core == 1)(lambda: pl.semaphore_wait(ready.at[0], 1))

    def others_here():
        def hear():
            pl.semaphore_wait(barrier, CORES * len(others))
            pl.semaphore_signal(ready.at[1], inc=1, device_id={"blk": partner})

        pl.when(core == 1)(hear)
        pl.when(core == 0)(lambda: pl.semaphore_wait(ready.at[1], 1))

    for one in small_loads:
        one.wait()
    within = lax.broadcasted_iota(jnp.int32, (1, group), 1)
    for g in range(2):
        own_group = table_ref[0, g]
        meta[me, pl.ds(g, 1), :] = doc_ref[pl.ds(own_group, 1), :].astype(jnp.float32)
        meta[me, pl.ds(2 + g, 1), :] = (own_group * group + within).astype(jnp.float32)
    cell_here()

    def remote(src, dst, ssem, rsem, target):
        return pltpu.make_async_remote_copy(
            src_ref=src, dst_ref=dst, send_sem=ssem, recv_sem=rsem, device_id={"blk": target}
        )

    def q_copy(cc, ch):
        return remote(stage_q.at[ch], qin.at[cell, chip], q_send, q_recv.at[cell, chip], index(cc, ch, core))

    def kv_copy(ch):
        place = own_slot(chip, core)
        return remote(stage_kv.at[ch], kv.at[place], kv_send, kv_recv.at[place], index(cell, ch, core))

    def kv_forward(ch):
        place = own_slot(ch, core)
        return remote(kv.at[place], kv.at[place], fwd_send, kv_recv.at[place], partner)

    def near_meta(ch):
        place = own_slot(chip, core)
        return remote(meta.at[me], meta.at[me], m_send, kv_recv.at[place], index(cell, ch, core))

    def far_meta(cc, ch):
        return remote(meta.at[me], meta.at[me], m_send, q_recv.at[cell, chip], index(cc, ch, core))

    def meta_forward(ch):
        source = index(cell, ch, core)
        return remote(meta.at[source], meta.at[source], mf_send, kv_recv.at[own_slot(ch, core)], partner)

    def await_all(ref, sem):
        pltpu.make_async_copy(ref, ref, sem).wait()

    def await_rows(count, sem):
        await_all(measure.at[pl.ds(0, count)], sem)

    meta_rows = 2 * meta.shape[1]

    def kv_arrival(place):
        await_rows(2 * rows + meta_rows, kv_recv.at[place])

    near = [one for one in peers if one[2] < heads]
    far = [one for one in peers if one[2] >= heads]
    for cc, ch, n in near:
        near_meta(ch).start()
    meta_forward(chip).start()
    await_all(stage_kv, load_kv)
    for cc, ch, n in near:
        kv_copy(ch).start()
    await_all(kv.at[own_slot(chip, core)], own_sem.at[0])
    kv_forward(chip).start()
    await_all(stage_q, load_q)
    others_here()
    for cc, ch, n in far:
        far_meta(cc, ch).start()
    for cc, ch, n in far:
        q_copy(cc, ch).start()
    for cc, ch, n in near:
        q_copy(cc, ch).start()
    own_q.wait()
    for cc, ch, n in near:
        kv_arrival(own_slot(ch, core))
        kv_forward(ch).start()
        meta_forward(ch).start()
    for i in range(heads):
        kv_arrival(own_slot(lax.rem(chip + i, heads), 1 - core))

    sources = heads * CORES
    down = lax.broadcasted_iota(jnp.int32, (group, group), 0)
    right = lax.broadcasted_iota(jnp.int32, (group, group), 1)
    diagonal = down == right

    def to_rows(line):
        return jnp.sum(jnp.where(diagonal, line, 0.0), axis=1, keepdims=True)

    def to_lanes(column):
        return jnp.sum(jnp.where(diagonal, column, 0.0), axis=0, keepdims=True)

    def attend(cc, ch, home):
        order = [lax.rem(own_slot(ch, core) + i, sources) for i in range(sources)]
        q = qin[cc, ch]
        doc_line = [meta[home, pl.ds(slot, 1), :] for slot in range(2)]
        pos_line = [meta[home, pl.ds(2 + slot, 1), :] for slot in range(2)]
        doc = [jnp.broadcast_to(to_rows(one), (group, group)) for one in doc_line]
        pos = [jnp.broadcast_to(to_rows(one), (group, group)) for one in pos_line]
        parts = [[], []]
        for g in range(2):
            part = pl.ds(g * group, group)
            keys = jnp.concatenate([kv[s, part, pl.ds(0, HEAD_DIM)] for s in order], axis=0)
            scores = lax.dot_general(
                q if g == 0 else q[group:], keys, (((1,), (1,)), ((), ())), preferred_element_type=jnp.float32
            )
            for i, s in enumerate(order):
                key_doc = meta[cell * sources + s, pl.ds(g, 1), :]
                key_pos = meta[cell * sources + s, pl.ds(2 + g, 1), :]
                for slot in range(g, 2):
                    row = (slot - g) * group
                    block = scores[row:row + group, i * group:(i + 1) * group]
                    if i:
                        seen = jnp.where(key_pos < pos_line[slot], key_doc, -1.0) == doc[slot]
                    else:
                        seen = (key_doc == doc[slot]) & (key_pos <= pos[slot])
                    parts[slot].append(jnp.where(seen, block, MASKED))
        best = []
        weights = []
        sums = []
        for slot in range(2):
            top = functools.reduce(jnp.maximum, parts[slot])
            top = jnp.broadcast_to(jnp.max(top, axis=1, keepdims=True), (group, group))
            found = [jnp.exp2((one - top) * factor) for one in parts[slot]]
            total = jnp.sum(functools.reduce(jnp.add, found), axis=1, keepdims=True)
            best.append(to_lanes(top))
            sums.append(to_lanes(jnp.broadcast_to(total, (group, group))))
            weights.append([one.astype(jnp.bfloat16) for one in found])
        outs = []
        for g in range(2):
            part = pl.ds(g * group, group)
            vals = jnp.concatenate([kv[s, part, pl.ds(HEAD_DIM, HEAD_DIM)] for s in order], axis=0)
            lines = [jnp.concatenate(weights[slot][g * sources:(g + 1) * sources], axis=1) for slot in range(g, 2)]
            line = lines[0] if g else jnp.concatenate(lines, axis=0)
            outs.append(jnp.dot(line, vals, preferred_element_type=jnp.float32))
        return (outs[0][:group], outs[0][group:] + outs[1]), best, sums

    def o_copy(cc, ch, n):
        return remote(osend.at[n], obuf.at[cell, chip], o_send, o_recv.at[cell, chip], index(cc, ch, core))

    def s_copy(cc, ch, n):
        return remote(ssend.at[n], sbuf.at[cell, chip], s_send, o_recv.at[cell, chip], index(cc, ch, core))

    cross_block = jnp.where(inner, 2, 3)
    own_block = jnp.where(inner, 3, 2)

    def place_of(t):
        block, step = t // half, lax.rem(t, half)
        is_cross, is_own = block == cross_block, block == own_block
        far_block = block - (cross_block < block).astype(jnp.int32) - (own_block < block).astype(jnp.int32)
        other = lax.rem(cell + 1 + far_block // 2, cells)
        far_layer = lax.rem(far_block + (inner).astype(jnp.int32), 2)
        far_chip = facing(other, far_layer * half + step)
        own_chip = layer * half + lax.rem(lax.rem(chip, half) + 1 + step, half)
        near_chip = jnp.where(is_own, own_chip, (1 - layer) * half + step)
        near_cell = is_cross | is_own
        return jnp.where(near_cell, cell, other), jnp.where(near_cell, near_chip, far_chip)

    def serve(t, carry):
        cc, ch = place_of(t)
        home = index(cc, ch, core)
        other = home != me

        pl.when((cc == cell) & other)(lambda: await_rows(rows, q_recv.at[cc, ch]))
        pl.when(cc != cell)(lambda: await_rows(rows + meta_rows, q_recv.at[cc, ch]))
        outs, best, sums = attend(cc, ch, home)
        for slot in range(2):
            osend[t, pl.ds(slot * group, group), :] = outs[slot].astype(jnp.bfloat16)
            ssend[t, pl.ds(slot, 1), :] = best[slot]
            ssend[t, pl.ds(2 + slot, 1), :] = sums[slot]

        def give():
            s_copy(cc, ch, t).start()
            o_copy(cc, ch, t).start()

        pl.when(other)(give)
        return carry

    lax.fori_loop(0, cells * heads, serve, 0)

    own_turn = own_block * half + half - 1
    obuf[cell, chip] = osend[own_turn]
    sbuf[cell, chip] = ssend[own_turn]

    for i in range(heads):
        h = lax.rem(layer * half + i, heads)
        for cc in range(cells):
            pl.when((cell != cc) | (chip != h))(lambda: await_rows(rows + meta_rows, o_recv.at[cc, h]))
        for slot in range(2):
            part = pl.ds(slot * group, group)
            tops = [sbuf[cc, h, pl.ds(slot, 1), :] for cc in range(cells)]
            sums = [sbuf[cc, h, pl.ds(2 + slot, 1), :] for cc in range(cells)]
            top = functools.reduce(jnp.maximum, tops)
            scale = [jnp.exp2((one - top) * factor) for one in tops]
            total = functools.reduce(jnp.add, [a * b for a, b in zip(scale, sums)])
            mixed = None
            for cc in range(cells):
                weight = to_rows(scale[cc] / total)
                term = obuf[cc, h, part, :].astype(jnp.float32) * weight
                mixed = term if mixed is None else mixed + term
            out_ref[part, head_columns(h)] = mixed.astype(out_ref.dtype)

    sent = pl.ds(0, cells * heads - 1)
    await_all(osend.at[sent], q_send)
    await_all(meta.at[sent], m_send)
    await_all(kv.at[pl.ds(0, heads - 1)], kv_send)
    await_all(kv.at[pl.ds(0, heads)], fwd_send)
    await_all(meta.at[pl.ds(0, heads)], mf_send)
    await_all(osend.at[sent], o_send)
    await_all(ssend.at[sent], s_send)


def solution(mesh):
    members = mesh.shape["blk"]

    def shards(queries, keys, values, group_table, doc_ids):
        rows, cols = queries.shape
        group = rows // 2
        heads = cols // HEAD_DIM
        cells = members // (heads * CORES)
        doc_rows = doc_ids.reshape(-1, group)
        bf16, f32 = jnp.bfloat16, jnp.float32
        dma = pltpu.SemaphoreType.DMA
        return pl.pallas_call(
            functools.partial(attend_kernel, cells),
            out_shape=jax.ShapeDtypeStruct((rows, cols), bf16),
            in_specs=[pl.BlockSpec(memory_space=pl.ANY)] * 5,
            out_specs=pl.BlockSpec(memory_space=pltpu.VMEM),
            scratch_shapes=[
                pltpu.SMEM((1, 2), jnp.int32),
                pltpu.VMEM(doc_rows.shape, jnp.int32),
                pltpu.VMEM((heads, rows, HEAD_DIM), bf16),
                pltpu.VMEM((heads, rows, 2 * HEAD_DIM), bf16),
                pltpu.VMEM((cells, heads, rows, HEAD_DIM), bf16),
                pltpu.VMEM((heads * CORES, rows, 2 * HEAD_DIM), bf16),
                pltpu.VMEM((members, 4, group), f32),
                pltpu.VMEM((cells * heads, rows, HEAD_DIM), bf16),
                pltpu.VMEM((cells * heads, 4, group), f32),
                pltpu.VMEM((cells, heads, rows, HEAD_DIM), bf16),
                pltpu.VMEM((cells, heads, 4, group), f32),
                pltpu.VMEM((2 * (rows + 4), HEAD_DIM), bf16),
                pltpu.SemaphoreType.REGULAR((2,)),
                dma((2,)),
                dma,
                dma,
                dma((2,)),
                dma,
                dma((cells, heads)),
                dma,
                dma((heads * CORES,)),
                dma,
                dma,
                dma,
                dma,
                dma,
                dma((cells, heads)),
            ],
            compiler_params=pltpu.CompilerParams(
                collective_id=0, has_side_effects=True, vmem_limit_bytes=12 * 1024 * 1024
            ),
        )(*[pltpu.with_memory_space_constraint(one, pltpu.HBM) for one in (group_table, queries, keys, values, doc_rows)])

    in_specs = (P("blk", "head"), P("blk", "head"), P("blk", "head"), P("blk", None), P())
    return jax.shard_map(shards, mesh=mesh, in_specs=in_specs, out_specs=P("blk", "head"), check_vma=False)
```

```python
import functools
import math

import jax
import jax.numpy as jnp
from jax import lax
from jax.experimental import pallas as pl
from jax.experimental.pallas import tpu as pltpu
from jax.sharding import PartitionSpec as P

HEAD_DIM = 128
CORES = 2
MASKED = -1e30


def attend_kernel(
    cells, table_hbm, q_hbm, k_hbm, v_hbm, doc_hbm, out_ref,
    table_ref, doc_ref, stage_q, stage_kv, qin, kv, meta, osend, ssend, obuf, sbuf, measure,
    ready, small_sem, load_q, load_kv, own_sem, q_send, q_recv, kv_send, kv_recv, m_send,
    o_send, s_send, o_recv,
):
    rows, cols = q_hbm.shape
    heads = cols // HEAD_DIM
    group = rows // 2
    factor = math.log2(math.e) / math.sqrt(HEAD_DIM)
    me = lax.axis_index("blk")
    core = lax.rem(me, CORES)
    chip = lax.rem(me // CORES, heads)
    cell = me // (CORES * heads)

    def index(cc, ch, co):
        return (cc * heads + ch) * CORES + co

    partner = index(cell, chip, 1 - core)

    half = heads // 2
    layer = chip // half
    inner = layer == (lax.rem(cell + 1, cells) > cell).astype(jnp.int32)

    def facing(other, i):
        return lax.rem(i + half * (other < cell).astype(jnp.int32), heads)

    def head_columns(h):
        start = h * HEAD_DIM
        if not isinstance(h, int):
            start = pl.multiple_of(start, HEAD_DIM)
        return pl.ds(start, HEAD_DIM)

    def own_slot(ch, co):
        return ch * CORES + co

    q_loads = [pltpu.make_async_copy(q_hbm.at[:, head_columns(h)], stage_q.at[h], load_q) for h in range(heads)]
    kv_loads = []
    for h in range(heads):
        for part, source in enumerate((k_hbm, v_hbm)):
            place = stage_kv.at[h, :, pl.ds(part * HEAD_DIM, HEAD_DIM)]
            kv_loads.append(pltpu.make_async_copy(source.at[:, head_columns(h)], place, load_kv))
    own_kv = [
        pltpu.make_async_copy(
            source.at[:, head_columns(chip)],
            kv.at[own_slot(chip, core), :, pl.ds(part * HEAD_DIM, HEAD_DIM)],
            own_sem.at[0],
        )
        for part, source in enumerate((k_hbm, v_hbm))
    ]
    own_q = pltpu.make_async_copy(q_hbm.at[:, head_columns(chip)], qin.at[cell, chip], own_sem.at[1])
    small_loads = (
        pltpu.make_async_copy(table_hbm, table_ref, small_sem.at[0]),
        pltpu.make_async_copy(doc_hbm, doc_ref, small_sem.at[1]),
    )
    for one in small_loads:
        one.start()
    for one in kv_loads:
        one.start()
    for one in own_kv:
        one.start()
    for one in q_loads:
        one.start()
    own_q.start()

    barrier = pltpu.get_barrier_semaphore()
    peers = []
    for i in range(heads - 1, 0, -1):
        peers.append((cell, chip ^ i, i))
    for k in range(1, cells):
        other = lax.rem(cell + k, cells)
        for i in range(heads):
            peers.append((other, facing(other, i) ^ lax.rem(chip, 2), k * heads + i))
    mates = [one for one in peers if one[2] < heads]
    others = [one for one in peers if one[2] >= heads]
    for cc, ch, _ in mates:
        pl.semaphore_signal(barrier, inc=1, device_id={"blk": index(cc, ch, 0)})
    for cc, ch, _ in others:
        pl.semaphore_signal(barrier, inc=1, device_id={"blk": index(cc, ch, 1)})

    pl.semaphore_signal(barrier, inc=1, device_id={"blk": partner})

    def cell_here():
        def hear():
            pl.semaphore_wait(barrier, CORES * len(mates) + 1)
            pl.semaphore_signal(ready.at[0], inc=1, device_id={"blk": partner})

        pl.when(core == 0)(hear)
        pl.when(core == 1)(lambda: pl.semaphore_wait(ready.at[0], 1))

    def others_here():
        def hear():
            pl.semaphore_wait(barrier, CORES * len(others) + 1)
            pl.semaphore_signal(ready.at[1], inc=1, device_id={"blk": partner})

        pl.when(core == 1)(hear)
        pl.when(core == 0)(lambda: pl.semaphore_wait(ready.at[1], 1))

    for one in small_loads:
        one.wait()
    within = lax.broadcasted_iota(jnp.int32, (1, group), 1)
    for g in range(2):
        own_group = table_ref[0, g]
        meta[me, pl.ds(g, 1), :] = doc_ref[pl.ds(own_group, 1), :].astype(jnp.float32)
        meta[me, pl.ds(2 + g, 1), :] = (own_group * group + within).astype(jnp.float32)
    cell_here()

    def remote(src, dst, ssem, rsem, target):
        return pltpu.make_async_remote_copy(
            src_ref=src, dst_ref=dst, send_sem=ssem, recv_sem=rsem, device_id={"blk": target}
        )

    def q_copy(cc, ch):
        return remote(stage_q.at[ch], qin.at[cell, chip], q_send, q_recv.at[cell, chip], index(cc, ch, core))

    def kv_copy(ch):
        place = own_slot(chip, core)
        return remote(stage_kv.at[ch], kv.at[place], kv_send, kv_recv.at[place], index(cell, ch, core))

    def kv_forward(ch):
        place = own_slot(ch, core)
        return remote(kv.at[place], kv.at[place], kv_send, kv_recv.at[place], partner)

    def near_meta(ch):
        place = own_slot(chip, core)
        return remote(meta.at[me], meta.at[me], m_send, kv_recv.at[place], index(cell, ch, core))

    def far_meta(cc, ch):
        return remote(meta.at[me], meta.at[me], m_send, q_recv.at[cell, chip], index(cc, ch, core))

    def meta_forward(ch):
        source = index(cell, ch, core)
        return remote(meta.at[source], meta.at[source], m_send, kv_recv.at[own_slot(ch, core)], partner)

    def await_all(ref, sem):
        pltpu.make_async_copy(ref, ref, sem).wait()

    def await_rows(count, sem):
        await_all(measure.at[pl.ds(0, count)], sem)

    meta_rows = 2 * meta.shape[1]

    def kv_arrival(place):
        await_rows(2 * rows + meta_rows, kv_recv.at[place])

    near = [one for one in peers if one[2] < heads]
    far = [one for one in peers if one[2] >= heads]
    for cc, ch, n in near:
        near_meta(ch).start()
    meta_forward(chip).start()
    await_all(stage_kv, load_kv)
    for cc, ch, n in near:
        kv_copy(ch).start()
    await_all(kv.at[own_slot(chip, core)], own_sem.at[0])
    kv_forward(chip).start()
    await_all(stage_q, load_q)
    others_here()
    for cc, ch, n in far:
        far_meta(cc, ch).start()
    for cc, ch, n in far:
        q_copy(cc, ch).start()
    for cc, ch, n in near:
        q_copy(cc, ch).start()
    own_q.wait()
    for cc, ch, n in near:
        kv_arrival(own_slot(ch, core))
        kv_forward(ch).start()
        meta_forward(ch).start()
    for i in range(heads):
        kv_arrival(own_slot(lax.rem(chip + i, heads), 1 - core))

    sources = heads * CORES
    down = lax.broadcasted_iota(jnp.int32, (group, group), 0)
    right = lax.broadcasted_iota(jnp.int32, (group, group), 1)
    diagonal = down == right

    def to_rows(line):
        return jnp.sum(jnp.where(diagonal, line, 0.0), axis=1, keepdims=True)

    def to_lanes(column):
        return jnp.sum(jnp.where(diagonal, column, 0.0), axis=0, keepdims=True)

    def attend(cc, ch, home):
        order = [lax.rem(own_slot(ch, core) + i, sources) for i in range(sources)]
        q = qin[cc, ch]
        doc_line = [meta[home, pl.ds(slot, 1), :] for slot in range(2)]
        pos_line = [meta[home, pl.ds(2 + slot, 1), :] for slot in range(2)]
        doc = [jnp.broadcast_to(to_rows(one), (group, group)) for one in doc_line]
        pos = [jnp.broadcast_to(to_rows(one), (group, group)) for one in pos_line]
        parts = [[], []]
        for g in range(2):
            part = pl.ds(g * group, group)
            keys = jnp.concatenate([kv[s, part, pl.ds(0, HEAD_DIM)] for s in order], axis=0)
            scores = lax.dot_general(
                q if g == 0 else q[group:], keys, (((1,), (1,)), ((), ())), preferred_element_type=jnp.float32
            )
            for i, s in enumerate(order):
                key_doc = meta[cell * sources + s, pl.ds(g, 1), :]
                key_pos = meta[cell * sources + s, pl.ds(2 + g, 1), :]
                for slot in range(g, 2):
                    row = (slot - g) * group
                    block = scores[row:row + group, i * group:(i + 1) * group]
                    if i:
                        seen = jnp.where(key_pos < pos_line[slot], key_doc, -1.0) == doc[slot]
                    else:
                        seen = (key_doc == doc[slot]) & (key_pos <= pos[slot])
                    parts[slot].append(jnp.where(seen, block, MASKED))
        best = []
        weights = []
        sums = []
        for slot in range(2):
            top = functools.reduce(jnp.maximum, parts[slot])
            top = jnp.broadcast_to(jnp.max(top, axis=1, keepdims=True), (group, group))
            found = [jnp.exp2((one - top) * factor) for one in parts[slot]]
            total = jnp.sum(functools.reduce(jnp.add, found), axis=1, keepdims=True)
            best.append(to_lanes(top))
            sums.append(to_lanes(jnp.broadcast_to(total, (group, group))))
            weights.append([one.astype(jnp.bfloat16) for one in found])
        outs = []
        for g in range(2):
            part = pl.ds(g * group, group)
            vals = jnp.concatenate([kv[s, part, pl.ds(HEAD_DIM, HEAD_DIM)] for s in order], axis=0)
            lines = [jnp.concatenate(weights[slot][g * sources:(g + 1) * sources], axis=1) for slot in range(g, 2)]
            line = lines[0] if g else jnp.concatenate(lines, axis=0)
            outs.append(jnp.dot(line, vals, preferred_element_type=jnp.float32))
        return (outs[0][:group], outs[0][group:] + outs[1]), best, sums

    def o_copy(cc, ch, n):
        return remote(osend.at[n], obuf.at[cell, chip], o_send, o_recv.at[cell, chip], index(cc, ch, core))

    def s_copy(cc, ch, n):
        return remote(ssend.at[n], sbuf.at[cell, chip], s_send, o_recv.at[cell, chip], index(cc, ch, core))

    cross_block = jnp.where(inner, 2, 3)
    own_block = jnp.where(inner, 3, 2)

    def place_of(t):
        block, step = t // half, lax.rem(t, half)
        is_cross, is_own = block == cross_block, block == own_block
        far_block = block - (cross_block < block).astype(jnp.int32) - (own_block < block).astype(jnp.int32)
        other = lax.rem(cell + 1 + far_block // 2, cells)
        far_layer = lax.rem(far_block + (inner).astype(jnp.int32), 2)
        far_chip = facing(other, far_layer * half + step)
        own_chip = layer * half + lax.rem(lax.rem(chip, half) + 1 + step, half)
        near_chip = jnp.where(is_own, own_chip, (1 - layer) * half + step)
        near_cell = is_cross | is_own
        return jnp.where(near_cell, cell, other), jnp.where(near_cell, near_chip, far_chip)

    def serve(t, carry):
        cc, ch = place_of(t)
        home = index(cc, ch, core)
        other = home != me

        pl.when((cc == cell) & other)(lambda: await_rows(rows, q_recv.at[cc, ch]))
        pl.when(cc != cell)(lambda: await_rows(rows + meta_rows, q_recv.at[cc, ch]))
        outs, best, sums = attend(cc, ch, home)
        for slot in range(2):
            osend[t, pl.ds(slot * group, group), :] = outs[slot].astype(jnp.bfloat16)
            ssend[t, pl.ds(slot, 1), :] = best[slot]
            ssend[t, pl.ds(2 + slot, 1), :] = sums[slot]

        def give():
            s_copy(cc, ch, t).start()
            o_copy(cc, ch, t).start()

        pl.when(other)(give)
        return carry

    lax.fori_loop(0, cells * heads, serve, 0)

    own_turn = own_block * half + half - 1
    obuf[cell, chip] = osend[own_turn]
    sbuf[cell, chip] = ssend[own_turn]

    for i in range(heads):
        h = lax.rem(layer * half + i, heads)
        for cc in range(cells):
            pl.when((cell != cc) | (chip != h))(lambda: await_rows(rows + meta_rows, o_recv.at[cc, h]))
        for slot in range(2):
            part = pl.ds(slot * group, group)
            tops = [sbuf[cc, h, pl.ds(slot, 1), :] for cc in range(cells)]
            sums = [sbuf[cc, h, pl.ds(2 + slot, 1), :] for cc in range(cells)]
            top = functools.reduce(jnp.maximum, tops)
            scale = [jnp.exp2((one - top) * factor) for one in tops]
            total = functools.reduce(jnp.add, [a * b for a, b in zip(scale, sums)])
            mixed = None
            for cc in range(cells):
                weight = to_rows(scale[cc] / total)
                term = obuf[cc, h, part, :].astype(jnp.float32) * weight
                mixed = term if mixed is None else mixed + term
            out_ref[part, head_columns(h)] = mixed.astype(out_ref.dtype)

    sent = pl.ds(0, cells * heads - 1)
    await_all(osend.at[sent], q_send)
    await_all(meta.at[pl.ds(0, cells * heads - 1 + heads)], m_send)
    await_all(kv.at[pl.ds(0, 2 * heads - 1)], kv_send)
    await_all(osend.at[sent], o_send)
    await_all(ssend.at[sent], s_send)


def solution(mesh):
    members = mesh.shape["blk"]

    def shards(queries, keys, values, group_table, doc_ids):
        rows, cols = queries.shape
        group = rows // 2
        heads = cols // HEAD_DIM
        cells = members // (heads * CORES)
        doc_rows = doc_ids.reshape(-1, group)
        bf16, f32 = jnp.bfloat16, jnp.float32
        dma = pltpu.SemaphoreType.DMA
        return pl.pallas_call(
            functools.partial(attend_kernel, cells),
            out_shape=jax.ShapeDtypeStruct((rows, cols), bf16),
            in_specs=[pl.BlockSpec(memory_space=pl.ANY)] * 5,
            out_specs=pl.BlockSpec(memory_space=pltpu.VMEM),
            scratch_shapes=[
                pltpu.SMEM((1, 2), jnp.int32),
                pltpu.VMEM(doc_rows.shape, jnp.int32),
                pltpu.VMEM((heads, rows, HEAD_DIM), bf16),
                pltpu.VMEM((heads, rows, 2 * HEAD_DIM), bf16),
                pltpu.VMEM((cells, heads, rows, HEAD_DIM), bf16),
                pltpu.VMEM((heads * CORES, rows, 2 * HEAD_DIM), bf16),
                pltpu.VMEM((members, 4, group), f32),
                pltpu.VMEM((cells * heads, rows, HEAD_DIM), bf16),
                pltpu.VMEM((cells * heads, 4, group), f32),
                pltpu.VMEM((cells, heads, rows, HEAD_DIM), bf16),
                pltpu.VMEM((cells, heads, 4, group), f32),
                pltpu.VMEM((2 * (rows + 4), HEAD_DIM), bf16),
                pltpu.SemaphoreType.REGULAR((2,)),
                dma((2,)),
                dma,
                dma,
                dma((2,)),
                dma,
                dma((cells, heads)),
                dma,
                dma((heads * CORES,)),
                dma,
                dma,
                dma,
                dma((cells, heads)),
            ],
            compiler_params=pltpu.CompilerParams(
                collective_id=0, has_side_effects=True, vmem_limit_bytes=12 * 1024 * 1024
            ),
        )(*[pltpu.with_memory_space_constraint(one, pltpu.HBM) for one in (group_table, queries, keys, values, doc_rows)])

    in_specs = (P("blk", "head"), P("blk", "head"), P("blk", "head"), P("blk", None), P())
    return jax.shard_map(shards, mesh=mesh, in_specs=in_specs, out_specs=P("blk", "head"), check_vma=False)
```

```python
import functools
import math

import jax
import jax.numpy as jnp
from jax import lax
from jax.experimental import pallas as pl
from jax.experimental.pallas import tpu as pltpu
from jax.sharding import PartitionSpec as P

HEAD_DIM = 128
CORES = 2
MASKED = -1e30


def attend_kernel(
    cells, table_hbm, q_hbm, k_hbm, v_hbm, doc_hbm, out_ref,
    table_ref, doc_ref, stage_q, stage_kv, qin, kv, meta, osend, ssend, obuf, sbuf, measure,
    ready, small_sem, load_q, load_kv, own_sem, q_send, q_recv, kv_send, kv_recv, m_send,
    o_send, s_send, o_recv,
):
    rows, cols = q_hbm.shape
    heads = cols // HEAD_DIM
    group = rows // 2
    factor = math.log2(math.e) / math.sqrt(HEAD_DIM)
    me = lax.axis_index("blk")
    core = lax.rem(me, CORES)
    chip = lax.rem(me // CORES, heads)
    cell = me // (CORES * heads)

    def index(cc, ch, co):
        return (cc * heads + ch) * CORES + co

    partner = index(cell, chip, 1 - core)

    half = heads // 2
    layer = chip // half
    inner = layer == (lax.rem(cell + 1, cells) > cell).astype(jnp.int32)

    def facing(other, i):
        return lax.rem(i + half * (other < cell).astype(jnp.int32), heads)

    def head_columns(h):
        start = h * HEAD_DIM
        if not isinstance(h, int):
            start = pl.multiple_of(start, HEAD_DIM)
        return pl.ds(start, HEAD_DIM)

    def own_slot(ch, co):
        return ch * CORES + co

    q_loads = [pltpu.make_async_copy(q_hbm.at[:, head_columns(h)], stage_q.at[h], load_q) for h in range(heads)]
    kv_loads = []
    for h in range(heads):
        for part, source in enumerate((k_hbm, v_hbm)):
            place = stage_kv.at[h, :, pl.ds(part * HEAD_DIM, HEAD_DIM)]
            kv_loads.append(pltpu.make_async_copy(source.at[:, head_columns(h)], place, load_kv))
    own_kv = [
        pltpu.make_async_copy(
            source.at[:, head_columns(chip)],
            kv.at[own_slot(chip, core), :, pl.ds(part * HEAD_DIM, HEAD_DIM)],
            own_sem.at[0],
        )
        for part, source in enumerate((k_hbm, v_hbm))
    ]
    own_q = pltpu.make_async_copy(q_hbm.at[:, head_columns(chip)], qin.at[cell, chip], own_sem.at[1])
    small_loads = (
        pltpu.make_async_copy(table_hbm, table_ref, small_sem.at[0]),
        pltpu.make_async_copy(doc_hbm, doc_ref, small_sem.at[1]),
    )
    for one in small_loads:
        one.start()
    for one in kv_loads:
        one.start()
    for one in own_kv:
        one.start()
    for one in q_loads:
        one.start()
    own_q.start()

    barrier = pltpu.get_barrier_semaphore()
    peers = []
    for i in range(heads - 1, 0, -1):
        peers.append((cell, chip ^ i, i))
    for k in range(1, cells):
        other = lax.rem(cell + k, cells)
        for i in range(heads):
            turned = jnp.where(inner, (i % 2) * half + i // 2, i)
            peers.append((other, facing(other, turned) ^ lax.rem(chip, 2), k * heads + i))
    mates = [one for one in peers if one[2] < heads]
    others = [one for one in peers if one[2] >= heads]
    for cc, ch, _ in mates:
        pl.semaphore_signal(barrier, inc=1, device_id={"blk": index(cc, ch, 0)})
    for cc, ch, _ in others:
        pl.semaphore_signal(barrier, inc=1, device_id={"blk": index(cc, ch, 1)})

    pl.semaphore_signal(barrier, inc=1, device_id={"blk": partner})

    def cell_here():
        def hear():
            pl.semaphore_wait(barrier, CORES * len(mates) + 1)
            pl.semaphore_signal(ready.at[0], inc=1, device_id={"blk": partner})

        pl.when(core == 0)(hear)
        pl.when(core == 1)(lambda: pl.semaphore_wait(ready.at[0], 1))

    def others_here():
        def hear():
            pl.semaphore_wait(barrier, CORES * len(others) + 1)
            pl.semaphore_signal(ready.at[1], inc=1, device_id={"blk": partner})

        pl.when(core == 1)(hear)
        pl.when(core == 0)(lambda: pl.semaphore_wait(ready.at[1], 1))

    for one in small_loads:
        one.wait()
    within = lax.broadcasted_iota(jnp.int32, (1, group), 1)
    for g in range(2):
        own_group = table_ref[0, g]
        meta[me, pl.ds(g, 1), :] = doc_ref[pl.ds(own_group, 1), :].astype(jnp.float32)
        meta[me, pl.ds(2 + g, 1), :] = (own_group * group + within).astype(jnp.float32)
    cell_here()

    def remote(src, dst, ssem, rsem, target):
        return pltpu.make_async_remote_copy(
            src_ref=src, dst_ref=dst, send_sem=ssem, recv_sem=rsem, device_id={"blk": target}
        )

    def q_copy(cc, ch):
        return remote(stage_q.at[ch], qin.at[cell, chip], q_send, q_recv.at[cell, chip], index(cc, ch, core))

    def kv_copy(ch):
        place = own_slot(chip, core)
        return remote(stage_kv.at[ch], kv.at[place], kv_send, kv_recv.at[place], index(cell, ch, core))

    def kv_forward(ch):
        place = own_slot(ch, core)
        return remote(kv.at[place], kv.at[place], kv_send, kv_recv.at[place], partner)

    def near_meta(ch):
        place = own_slot(chip, core)
        return remote(meta.at[me], meta.at[me], m_send, kv_recv.at[place], index(cell, ch, core))

    def far_meta(cc, ch):
        return remote(meta.at[me], meta.at[me], m_send, q_recv.at[cell, chip], index(cc, ch, core))

    def meta_forward(ch):
        source = index(cell, ch, core)
        return remote(meta.at[source], meta.at[source], m_send, kv_recv.at[own_slot(ch, core)], partner)

    def await_all(ref, sem):
        pltpu.make_async_copy(ref, ref, sem).wait()

    def await_rows(count, sem):
        await_all(measure.at[pl.ds(0, count)], sem)

    meta_rows = 2 * meta.shape[1]

    def kv_arrival(place):
        await_rows(2 * rows + meta_rows, kv_recv.at[place])

    near = [one for one in peers if one[2] < heads]
    far = [one for one in peers if one[2] >= heads]
    for cc, ch, n in near:
        near_meta(ch).start()
    meta_forward(chip).start()
    await_all(stage_kv, load_kv)
    for cc, ch, n in near:
        kv_copy(ch).start()
    await_all(kv.at[own_slot(chip, core)], own_sem.at[0])
    kv_forward(chip).start()
    await_all(stage_q, load_q)
    others_here()
    for cc, ch, n in far:
        far_meta(cc, ch).start()
    for cc, ch, n in far:
        q_copy(cc, ch).start()
    for cc, ch, n in near:
        q_copy(cc, ch).start()
    own_q.wait()
    for cc, ch, n in near:
        kv_arrival(own_slot(ch, core))
        kv_forward(ch).start()
        meta_forward(ch).start()
    for i in range(heads):
        kv_arrival(own_slot(lax.rem(chip + i, heads), 1 - core))

    sources = heads * CORES
    down = lax.broadcasted_iota(jnp.int32, (group, group), 0)
    right = lax.broadcasted_iota(jnp.int32, (group, group), 1)
    diagonal = down == right

    def to_rows(line):
        return jnp.sum(jnp.where(diagonal, line, 0.0), axis=1, keepdims=True)

    def to_lanes(column):
        return jnp.sum(jnp.where(diagonal, column, 0.0), axis=0, keepdims=True)

    def attend(cc, ch, home):
        order = [lax.rem(own_slot(ch, core) + i, sources) for i in range(sources)]
        q = qin[cc, ch]
        doc_line = [meta[home, pl.ds(slot, 1), :] for slot in range(2)]
        pos_line = [meta[home, pl.ds(2 + slot, 1), :] for slot in range(2)]
        doc = [jnp.broadcast_to(to_rows(one), (group, group)) for one in doc_line]
        pos = [jnp.broadcast_to(to_rows(one), (group, group)) for one in pos_line]
        parts = [[], []]
        for g in range(2):
            part = pl.ds(g * group, group)
            keys = jnp.concatenate([kv[s, part, pl.ds(0, HEAD_DIM)] for s in order], axis=0)
            scores = lax.dot_general(
                q if g == 0 else q[group:], keys, (((1,), (1,)), ((), ())), preferred_element_type=jnp.float32
            )
            for i, s in enumerate(order):
                key_doc = meta[cell * sources + s, pl.ds(g, 1), :]
                key_pos = meta[cell * sources + s, pl.ds(2 + g, 1), :]
                for slot in range(g, 2):
                    row = (slot - g) * group
                    block = scores[row:row + group, i * group:(i + 1) * group]
                    if i:
                        seen = jnp.where(key_pos < pos_line[slot], key_doc, -1.0) == doc[slot]
                    else:
                        seen = (key_doc == doc[slot]) & (key_pos <= pos[slot])
                    parts[slot].append(jnp.where(seen, block, MASKED))
        best = []
        weights = []
        sums = []
        for slot in range(2):
            top = functools.reduce(jnp.maximum, parts[slot])
            top = jnp.broadcast_to(jnp.max(top, axis=1, keepdims=True), (group, group))
            found = [jnp.exp2((one - top) * factor) for one in parts[slot]]
            total = jnp.sum(functools.reduce(jnp.add, found), axis=1, keepdims=True)
            best.append(to_lanes(top))
            sums.append(to_lanes(jnp.broadcast_to(total, (group, group))))
            weights.append([one.astype(jnp.bfloat16) for one in found])
        outs = []
        for g in range(2):
            part = pl.ds(g * group, group)
            vals = jnp.concatenate([kv[s, part, pl.ds(HEAD_DIM, HEAD_DIM)] for s in order], axis=0)
            lines = [jnp.concatenate(weights[slot][g * sources:(g + 1) * sources], axis=1) for slot in range(g, 2)]
            line = lines[0] if g else jnp.concatenate(lines, axis=0)
            outs.append(jnp.dot(line, vals, preferred_element_type=jnp.float32))
        return (outs[0][:group], outs[0][group:] + outs[1]), best, sums

    def o_copy(cc, ch, n):
        return remote(osend.at[n], obuf.at[cell, chip], o_send, o_recv.at[cell, chip], index(cc, ch, core))

    def s_copy(cc, ch, n):
        return remote(ssend.at[n], sbuf.at[cell, chip], s_send, o_recv.at[cell, chip], index(cc, ch, core))

    cross_block = jnp.where(inner, 2, 3)
    own_block = jnp.where(inner, 3, 2)

    def place_of(t):
        block, step = t // half, lax.rem(t, half)
        is_cross, is_own = block == cross_block, block == own_block
        far_block = block - (cross_block < block).astype(jnp.int32) - (own_block < block).astype(jnp.int32)
        other = lax.rem(cell + 1 + far_block // 2, cells)
        far_layer = lax.rem(far_block + (inner).astype(jnp.int32), 2)
        far_chip = facing(other, far_layer * half + step)
        own_chip = layer * half + lax.rem(lax.rem(chip, half) + 1 + step, half)
        near_chip = jnp.where(is_own, own_chip, (1 - layer) * half + step)
        near_cell = is_cross | is_own
        return jnp.where(near_cell, cell, other), jnp.where(near_cell, near_chip, far_chip)

    def serve(t, carry):
        cc, ch = place_of(t)
        home = index(cc, ch, core)
        other = home != me

        pl.when((cc == cell) & other)(lambda: await_rows(rows, q_recv.at[cc, ch]))
        pl.when(cc != cell)(lambda: await_rows(rows + meta_rows, q_recv.at[cc, ch]))
        outs, best, sums = attend(cc, ch, home)
        for slot in range(2):
            osend[t, pl.ds(slot * group, group), :] = outs[slot].astype(jnp.bfloat16)
            ssend[t, pl.ds(slot, 1), :] = best[slot]
            ssend[t, pl.ds(2 + slot, 1), :] = sums[slot]

        def give():
            s_copy(cc, ch, t).start()
            o_copy(cc, ch, t).start()

        pl.when(other)(give)
        return carry

    lax.fori_loop(0, cells * heads, serve, 0)

    own_turn = own_block * half + half - 1
    obuf[cell, chip] = osend[own_turn]
    sbuf[cell, chip] = ssend[own_turn]

    for i in range(heads):
        h = lax.rem(layer * half + i, heads)
        for cc in range(cells):
            pl.when((cell != cc) | (chip != h))(lambda: await_rows(rows + meta_rows, o_recv.at[cc, h]))
        for slot in range(2):
            part = pl.ds(slot * group, group)
            tops = [sbuf[cc, h, pl.ds(slot, 1), :] for cc in range(cells)]
            sums = [sbuf[cc, h, pl.ds(2 + slot, 1), :] for cc in range(cells)]
            top = functools.reduce(jnp.maximum, tops)
            scale = [jnp.exp2((one - top) * factor) for one in tops]
            total = functools.reduce(jnp.add, [a * b for a, b in zip(scale, sums)])
            mixed = None
            for cc in range(cells):
                weight = to_rows(scale[cc] / total)
                term = obuf[cc, h, part, :].astype(jnp.float32) * weight
                mixed = term if mixed is None else mixed + term
            out_ref[part, head_columns(h)] = mixed.astype(out_ref.dtype)

    sent = pl.ds(0, cells * heads - 1)
    await_all(osend.at[sent], q_send)
    await_all(meta.at[pl.ds(0, cells * heads - 1 + heads)], m_send)
    await_all(kv.at[pl.ds(0, 2 * heads - 1)], kv_send)
    await_all(osend.at[sent], o_send)
    await_all(ssend.at[sent], s_send)


def solution(mesh):
    members = mesh.shape["blk"]

    def shards(queries, keys, values, group_table, doc_ids):
        rows, cols = queries.shape
        group = rows // 2
        heads = cols // HEAD_DIM
        cells = members // (heads * CORES)
        doc_rows = doc_ids.reshape(-1, group)
        bf16, f32 = jnp.bfloat16, jnp.float32
        dma = pltpu.SemaphoreType.DMA
        return pl.pallas_call(
            functools.partial(attend_kernel, cells),
            out_shape=jax.ShapeDtypeStruct((rows, cols), bf16),
            in_specs=[pl.BlockSpec(memory_space=pl.ANY)] * 5,
            out_specs=pl.BlockSpec(memory_space=pltpu.VMEM),
            scratch_shapes=[
                pltpu.SMEM((1, 2), jnp.int32),
                pltpu.VMEM(doc_rows.shape, jnp.int32),
                pltpu.VMEM((heads, rows, HEAD_DIM), bf16),
                pltpu.VMEM((heads, rows, 2 * HEAD_DIM), bf16),
                pltpu.VMEM((cells, heads, rows, HEAD_DIM), bf16),
                pltpu.VMEM((heads * CORES, rows, 2 * HEAD_DIM), bf16),
                pltpu.VMEM((members, 4, group), f32),
                pltpu.VMEM((cells * heads, rows, HEAD_DIM), bf16),
                pltpu.VMEM((cells * heads, 4, group), f32),
                pltpu.VMEM((cells, heads, rows, HEAD_DIM), bf16),
                pltpu.VMEM((cells, heads, 4, group), f32),
                pltpu.VMEM((2 * (rows + 4), HEAD_DIM), bf16),
                pltpu.SemaphoreType.REGULAR((2,)),
                dma((2,)),
                dma,
                dma,
                dma((2,)),
                dma,
                dma((cells, heads)),
                dma,
                dma((heads * CORES,)),
                dma,
                dma,
                dma,
                dma((cells, heads)),
            ],
            compiler_params=pltpu.CompilerParams(
                collective_id=0, has_side_effects=True, vmem_limit_bytes=12 * 1024 * 1024
            ),
        )(*[pltpu.with_memory_space_constraint(one, pltpu.HBM) for one in (group_table, queries, keys, values, doc_rows)])

    in_specs = (P("blk", "head"), P("blk", "head"), P("blk", "head"), P("blk", None), P())
    return jax.shard_map(shards, mesh=mesh, in_specs=in_specs, out_specs=P("blk", "head"), check_vma=False)
```
